64 devices in a mesh: dp: 4 (over x, y), sp: 16 (over z, core).
Axes of the slice: x: 2, y: 2, z: 8, core: 2. Of those that a mesh axis runs over, the one named last changes fastest.
The devices are a block of a 4x4x8 slice.
Arguments:
- images: bfloat16 [128, 32, 256, 128], P('dp', 'sp'), parts along dimension 0
- w_a: bfloat16 [2, 3, 3, 128, 128], replicated
- bn_a: float32 [2, 2, 128], replicated
- w_down: bfloat16 [3, 3, 128, 1024], replicated
- bn_down: float32 [2, 1024], replicated
- w_in: bfloat16 [3, 1024, 256], replicated
- bn_in: float32 [3, 2, 256], replicated
- w_mid: bfloat16 [3, 3, 3, 256, 256], replicated
- bn_mid: float32 [3, 2, 256], replicated
- w_out: bfloat16 [3, 256, 1024], replicated
- bn_out: float32 [3, 2, 1024], replicated
Outputs:
- output: bfloat16 [128, 16, 128, 1024], P('dp', 'sp'), parts along dimension 0
There are 4 independent parts. The reference program is written for one: setup_inputs(seed, part) draws one part's arguments, and reference() takes and returns one part's arrays. A program takes and returns all parts, laid end to end along the dimension named above; an argument that names none is the same for every part.
All inputs are finite; a program needn't handle non-finite values.
Results may differ from the reference program's by a relative error of at most 0.02.
Values are sent between devices in bfloat16 or wider.
A program may use at most 768 MiB of HBM per device.

```python
import jax
import jax.numpy as jnp
from jax import lax

IMAGES = 32
ROWS_DEV = 2
IMG_WIDTH = 256
LAYERS_A = 2
BLOCKS_B = 3
CHAN_A = 128
CHAN_MID = 256
CHAN_B = 1024
GROUP_SIZE = 16
NORM_EPS = 1e-5
CONV_DIMS = ("NHWC", "HWIO", "NHWC")


def conv_weight(draw_key, full_shape, fan_in):
    return (jax.random.normal(draw_key, full_shape, jnp.float32) * fan_in ** -0.5).astype(jnp.bfloat16)


def norm_params(draw_key, lead_dims, chan_count):
    key_gain, key_shift = jax.random.split(draw_key)
    norm_gain = jax.random.uniform(key_gain, lead_dims + (chan_count,), jnp.float32, 0.6, 1.4)
    norm_shift = 0.4 * jax.random.normal(key_shift, lead_dims + (chan_count,), jnp.float32)
    return jnp.stack([norm_gain, norm_shift], axis=-2)


def setup_inputs(seed: int = 0, part: int = 0) -> dict:
    base_key = jax.random.key(seed)
    part_key = jax.random.fold_in(base_key, part)
    key_noise, key_amp, key_phase = jax.random.split(part_key, 3)
    weight_keys = jax.random.split(base_key, 10)
    height = GROUP_SIZE * ROWS_DEV
    row_pos = (jnp.arange(height, dtype=jnp.float32) + 0.5) / height
    band_amp = 1.5 * jax.random.normal(key_amp, (CHAN_A,), jnp.float32)
    band_phase = 6.2832 * jax.random.uniform(key_phase, (CHAN_A,), jnp.float32)
    row_band = band_amp * (1.0 - 2.0 * row_pos)[:, None] + jnp.sin(12.566 * row_pos[:, None] + band_phase)
    pixel_noise = jax.random.normal(key_noise, (IMAGES, height, IMG_WIDTH, CHAN_A), jnp.float32)
    return {
        "images": (pixel_noise + row_band[None, :, None, :]).astype(jnp.bfloat16),
        "w_a": conv_weight(weight_keys[0], (LAYERS_A, 3, 3, CHAN_A, CHAN_A), 9 * CHAN_A),
        "bn_a": norm_params(weight_keys[1], (LAYERS_A,), CHAN_A),
        "w_down": conv_weight(weight_keys[2], (3, 3, CHAN_A, CHAN_B), 9 * CHAN_A),
        "bn_down": norm_params(weight_keys[3], (), CHAN_B),
        "w_in": conv_weight(weight_keys[4], (BLOCKS_B, CHAN_B, CHAN_MID), CHAN_B),
        "bn_in": norm_params(weight_keys[5], (BLOCKS_B,), CHAN_MID),
        "w_mid": conv_weight(weight_keys[6], (BLOCKS_B, 3, 3, CHAN_MID, CHAN_MID), 9 * CHAN_MID),
        "bn_mid": norm_params(weight_keys[7], (BLOCKS_B,), CHAN_MID),
        "w_out": conv_weight(weight_keys[8], (BLOCKS_B, CHAN_MID, CHAN_B), CHAN_MID),
        "bn_out": norm_params(weight_keys[9], (BLOCKS_B,), CHAN_B),
    }


def conv_full(hidden, weight, stride):
    return lax.conv_general_dilated(hidden.astype(jnp.float32), weight.astype(jnp.float32), (stride, stride), "SAME", dimension_numbers=CONV_DIMS)


def conv_point(hidden, weight):
    return jnp.einsum("bhwc,cd->bhwd", hidden.astype(jnp.float32), weight.astype(jnp.float32))


def batch_norm(pre_act, params):
    chan_mean = jnp.mean(pre_act, axis=(0, 1, 2))
    chan_var = jnp.mean(pre_act * pre_act, axis=(0, 1, 2)) - chan_mean * chan_mean
    chan_scale = params[0] * lax.rsqrt(chan_var + NORM_EPS)
    return (pre_act - chan_mean) * chan_scale + params[1]


def norm_relu(pre_act, params):
    return jax.nn.relu(batch_norm(pre_act, params)).astype(jnp.bfloat16)


def reference(images, w_a, bn_a, w_down, bn_down, w_in, bn_in, w_mid, bn_mid, w_out, bn_out):
    def stage_a(hidden, layer_args):
        return norm_relu(conv_full(hidden, layer_args[0], 1), layer_args[1]), None

    def bottleneck(hidden, block_args):
        w_first, bn_first, w_three, bn_three, w_last, bn_last = block_args
        branch = norm_relu(conv_point(hidden, w_first), bn_first)
        branch = norm_relu(conv_full(branch, w_three, 1), bn_three)
        summed = batch_norm(conv_point(branch, w_last), bn_last) + hidden.astype(jnp.float32)
        return jax.nn.relu(summed).astype(jnp.bfloat16), None

    hidden, _ = lax.scan(stage_a, images, (w_a, bn_a))
    hidden = norm_relu(conv_full(hidden, w_down, 2), bn_down)
    hidden, _ = lax.scan(bottleneck, hidden, (w_in, bn_in, w_mid, bn_mid, w_out, bn_out))
    return hidden
```

```python
import jax
import jax.numpy as jnp
from jax import lax
from jax.experimental import pallas as pl
from jax.experimental.pallas import tpu as pltpu
from jax.sharding import PartitionSpec as P

NORM_EPS = 1e-5
CHUNKS = 8
TILE = 256
F32 = jnp.float32
BF16 = jnp.bfloat16


def solution(mesh):
    groups = mesh.shape["sp"]
    peers = sorted(range(1, groups), key=lambda k: (abs(2 * k - groups), k))

    def make_kernel(batch, rows, width, chan_a, chan_b, chan_m, layers, blocks):
        half_w = width // 2
        points = batch * half_w
        per_chunk = batch // CHUNKS
        half_b = batch // 2
        tiles = chan_b // TILE
        m_rows = points // CHUNKS
        count_a = float(batch * rows * width * groups)
        count_b = float(points * groups)
        ar_down = layers
        ar_in = ar_down + tiles
        ar_mid = ar_in + blocks
        ar_out = ar_mid + blocks
        ar_total = ar_out + blocks * tiles

        def kernel(images, w_a, w_down, w_in, w_mid, w_out, bn_a, bn_down, bn_in, bn_mid, bn_out, out,
                   xa, u, zb, h, u2, wa, wd, win, wmid, wout, st, nrm, tmp, arsend, arbuf,
                   sem_w, sem_img, a_send, a_recv, u_send, u_recv, ar_ssem, ar_rsem, sem_out):
            me = lax.axis_index("sp")
            has_prev = me > 0
            has_next = me < groups - 1
            prev = jnp.maximum(me - 1, 0)
            nxt = jnp.minimum(me + 1, groups - 1)

            def remote(src, dst, ssem, rsem, dev):
                return pltpu.make_async_remote_copy(src_ref=src, dst_ref=dst, send_sem=ssem, recv_sem=rsem,
                                                    device_id={"sp": dev}, device_id_type=pl.DeviceIdType.MESH)

            def img_copy(c, r):
                sl = pl.ds(c * per_chunk, per_chunk)
                return pltpu.make_async_copy(images.at[sl, r], xa.at[1 + r, sl], sem_img.at[r, c])

            def load_images(c, _):
                for r in range(2):
                    img_copy(c, r).start()
                return 0
            for dy in range(3):
                for dx in range(3):
                    for l in range(layers):
                        pltpu.make_async_copy(w_a.at[l, dy, dx], wa.at[l, pl.ds(dy * chan_a, chan_a), pl.ds(dx * chan_a, chan_a)], sem_w.at[0]).start()
            lax.fori_loop(0, CHUNKS, load_images, 0)

            barrier = pltpu.get_barrier_semaphore()
            for k in peers:
                pl.semaphore_signal(barrier, inc=1, device_id={"sp": lax.rem(me + k, groups)}, device_id_type=pl.DeviceIdType.MESH)
            pl.semaphore_wait(barrier, groups - 1)

            def a_copies(c, first):
                sl = pl.ds(c * per_chunk, per_chunk)
                top = images.at[sl, 0] if first else xa.at[1, sl]
                bot = images.at[sl, 1] if first else xa.at[2, sl]
                up = remote(top, xa.at[3, sl], a_send.at[0, c], a_recv.at[1, c], prev)
                down = remote(bot, xa.at[0, sl], a_send.at[1, c], a_recv.at[0, c], nxt)
                return up, down

            def d_copy(c):
                sl = pl.ds(c * per_chunk, per_chunk)
                return remote(u.at[0, sl], u.at[2, sl], u_send.at[0, c], u_recv.at[1, c], prev)

            def u_copies(c):
                sl = pl.ds(c * per_chunk, per_chunk)
                up = remote(u.at[1, sl], u.at[2, sl], u_send.at[0, c], u_recv.at[1, c], prev)
                down = remote(u.at[1, sl], u.at[0, sl], u_send.at[1, c], u_recv.at[0, c], nxt)
                return up, down

            def start_pair(up, down):
                @pl.when(has_prev)
                def _():
                    up.start()

                @pl.when(has_next)
                def _():
                    down.start()

            def wait_sends(pair_of):
                def body(c, _):
                    up, down = pair_of(c)

                    @pl.when(has_prev)
                    def _():
                        up.wait_send()

                    @pl.when(has_next)
                    def _():
                        down.wait_send()
                    return 0
                lax.fori_loop(0, CHUNKS, body, 0)

            def wait_halo(pair_of, c):
                up, down = pair_of(c)

                @pl.when(has_prev)
                def _():
                    down.wait_recv()

                @pl.when(has_next)
                def _():
                    up.wait_recv()

            def clear_moments():
                st[...] = jnp.zeros_like(st)

            def add_moments(z, lo):
                wide = z.shape[-1]
                z8 = z.reshape(z.shape[0] // 8, 8, wide)
                st[0, :, lo:lo + wide] += jnp.sum(z8, axis=0)
                st[1, :, lo:lo + wide] += jnp.sum(z8 * z8, axis=0)

            def ar_copy(a, k):
                return remote(arsend.at[a], arbuf.at[a, k - 1], ar_ssem.at[a], ar_rsem.at[a], lax.rem(me + k, groups))

            def send_moments(a, lo, wide):
                s = jnp.sum(st[0, :, lo:lo + wide], axis=0, keepdims=True)
                q = jnp.sum(st[1, :, lo:lo + wide], axis=0, keepdims=True)
                both = jnp.concatenate([s, q] * (TILE // wide), axis=1)
                arsend[a] = both
                for k in peers:
                    ar_copy(a, k).start()

            def recv_moments(a, params, lo, wide, count):
                pltpu.make_async_copy(arbuf.at[a], arbuf.at[a], ar_rsem.at[a]).wait()
                total = jnp.sum(arbuf[a], axis=0) + arsend[a]
                m = total[:, :wide] / count
                q = total[:, wide:2 * wide] / count
                v = q - m * m
                nrm[0:1, lo:lo + wide] = m
                nrm[1:2, lo:lo + wide] = params[0:1] * lax.rsqrt(v + NORM_EPS)
                nrm[2:3, lo:lo + wide] = params[1:2]
                pltpu.make_async_copy(arbuf.at[a], arbuf.at[a], ar_ssem.at[a]).wait()

            def norm(z, lo):
                wide = z.shape[-1]
                return (z - nrm[0:1, lo:lo + wide]) * nrm[1:2, lo:lo + wide] + nrm[2:3, lo:lo + wide]

            def norm_relu(z, lo):
                return jnp.maximum(norm(z, lo), 0.0)

            def from_left(y, wide):
                col = lax.broadcasted_iota(jnp.int32, y.shape, 0)
                return jnp.where(lax.rem(col, wide) == 0, 0.0, pltpu.roll(y, 1, 0))

            def from_right(y, wide):
                col = lax.broadcasted_iota(jnp.int32, y.shape, 0)
                return jnp.where(lax.rem(col, wide) == wide - 1, 0.0, pltpu.roll(y, y.shape[0] - 1, 0))

            def dot(x, w):
                return jnp.dot(x, w, preferred_element_type=F32)

            @pl.when(me == 0)
            def _():
                def body(b, _):
                    xa[0, b] = jnp.zeros((width, chan_a), BF16)
                    return 0
                lax.fori_loop(0, batch, body, 0)

            @pl.when(me == groups - 1)
            def _():
                def body(b, _):
                    xa[3, b] = jnp.zeros((width, chan_a), BF16)
                    u[2, b] = jnp.zeros((half_w, 2 * chan_a), BF16)
                    return 0
                lax.fori_loop(0, batch, body, 0)

            def send_a(c, _):
                start_pair(*a_copies(c, True))
                return 0
            lax.fori_loop(0, CHUNKS, send_a, 0)

            for dy in range(3):
                for dx in range(3):
                    row = (2 * dy + dx) * chan_a if dx < 2 else (6 + dy) * chan_a
                    pltpu.make_async_copy(w_down.at[dy, dx], wd.at[pl.ds(row, chan_a)], sem_w.at[1]).start()
                    for j in range(blocks):
                        pltpu.make_async_copy(w_mid.at[j, dy, dx], wmid.at[j, pl.ds(dy * chan_m, chan_m), pl.ds(dx * chan_m, chan_m)], sem_w.at[3]).start()
            pltpu.make_async_copy(w_in, win, sem_w.at[2]).start()
            pltpu.make_async_copy(w_out, wout, sem_w.at[4]).start()

            def wait_weight(ref, i):
                pltpu.make_async_copy(ref, ref, sem_w.at[i]).wait()

            wait_weight(wa, 0)

            def conv_a(l):
                clear_moments()
                for hb in range(2):
                    def body(i, _):
                        b = hb * half_b + i
                        c = b // per_chunk

                        @pl.when(lax.rem(b, per_chunk) == 0)
                        def _():
                            if l == 0:
                                for r in range(2):
                                    img_copy(c, r).wait()
                            wait_halo(lambda c: a_copies(c, l == 0), c)
                        for r in range(2):
                            x = jnp.concatenate([xa[r, b], xa[r + 1, b], xa[r + 2, b]], axis=1)
                            z = dot(x, wa[l, :, chan_a:2 * chan_a])
                            z = z + from_left(dot(x, wa[l, :, 0:chan_a]), width)
                            z = z + from_right(dot(x, wa[l, :, 2 * chan_a:3 * chan_a]), width)
                            lane = (2 * r + hb) * chan_a
                            zb[pl.ds(pl.multiple_of(i * width, width), width), lane:lane + chan_a] = z
                            add_moments(z, 0)
                        return 0
                    lax.fori_loop(0, half_b, body, 0)
                send_moments(l, 0, chan_a)
                wait_sends(lambda c: a_copies(c, l == 0))
                recv_moments(l, bn_a[l], 0, chan_a, count_a)

            conv_a(0)
            for l in range(1, layers):
                for hb in range(2):
                    def renorm(i, _):
                        b = hb * half_b + i
                        for r in range(2):
                            lane = (2 * r + hb) * chan_a
                            z = zb[pl.ds(pl.multiple_of(i * width, width), width), lane:lane + chan_a]
                            xa[1 + r, b] = norm_relu(z, 0).astype(BF16)

                        @pl.when(lax.rem(b, per_chunk) == per_chunk - 1)
                        def _():
                            start_pair(*a_copies(b // per_chunk, False))
                        return 0
                    lax.fori_loop(0, half_b, renorm, 0)
                conv_a(l)

            for hb in range(2):
                def pair_up(i, _):
                    b = hb * half_b + i
                    for r in range(2):
                        lane = (2 * r + hb) * chan_a
                        z = zb[pl.ds(pl.multiple_of(i * width, width), width), lane:lane + chan_a]
                        tmp[r] = norm_relu(z, 0)
                        u[r, b, :, 0:chan_a] = tmp[r, pl.ds(0, half_w, stride=2), :].astype(BF16)
                        u[r, b, :, chan_a:2 * chan_a] = tmp[r, pl.ds(1, half_w, stride=2), :].astype(BF16)

                    @pl.when(jnp.logical_and(lax.rem(b, per_chunk) == per_chunk - 1, has_prev))
                    def _():
                        d_copy(b // per_chunk).start()
                    return 0
                lax.fori_loop(0, half_b, pair_up, 0)

            wait_weight(wd, 1)
            clear_moments()

            def down_body(c, _):
                @pl.when(has_next)
                def _():
                    d_copy(c).wait_recv()
                sl = pl.ds(c * per_chunk, per_chunk)
                flat = [u[r, sl].reshape(m_rows, 2 * chan_a) for r in range(3)]
                evens = [from_right(f[:, :chan_a].astype(F32), half_w).astype(BF16) for f in flat]
                x = jnp.concatenate(flat + evens, axis=1)
                rows_at = pl.ds(pl.multiple_of(c * m_rows, m_rows), m_rows)
                for t in range(tiles):
                    z = dot(x, wd[:, t * TILE:(t + 1) * TILE])
                    zb[rows_at, t * TILE:(t + 1) * TILE] = z
                    add_moments(z, t * TILE)
                return 0
            lax.fori_loop(0, CHUNKS, down_body, 0)
            for t in range(tiles):
                send_moments(ar_down + t, t * TILE, TILE)

            def wait_d(c, _):
                @pl.when(has_prev)
                def _():
                    d_copy(c).wait_send()
                return 0
            lax.fori_loop(0, CHUNKS, wait_d, 0)

            @pl.when(me == 0)
            def _():
                def body(b, _):
                    u[0, b] = jnp.zeros((half_w, chan_m), BF16)
                    return 0
                lax.fori_loop(0, batch, body, 0)

            for t in range(tiles):
                cols = slice(t * TILE, (t + 1) * TILE)
                recv_moments(ar_down + t, bn_down[:, cols], t * TILE, TILE, count_b)

                def first_h(c, _):
                    rows_at = pl.ds(pl.multiple_of(c * m_rows, m_rows), m_rows)
                    h[rows_at, cols] = norm_relu(zb[rows_at, cols], t * TILE).astype(BF16)
                    return 0
                lax.fori_loop(0, CHUNKS, first_h, 0)

            wait_weight(win, 2)
            wait_weight(wmid, 3)
            wait_weight(wout, 4)

            def block(j, _):
                clear_moments()

                def in_body(c, _):
                    rows_at = pl.ds(pl.multiple_of(c * m_rows, m_rows), m_rows)
                    z = dot(h[rows_at, :], win[j])
                    zb[rows_at, 0:chan_m] = z
                    add_moments(z, 0)
                    return 0
                lax.fori_loop(0, CHUNKS, in_body, 0)
                send_moments(ar_in + j, 0, chan_m)
                recv_moments(ar_in + j, bn_in[j], 0, chan_m, count_b)

                def renorm_u(c, _):
                    rows_at = pl.ds(pl.multiple_of(c * m_rows, m_rows), m_rows)
                    sl = pl.ds(c * per_chunk, per_chunk)
                    u[1, sl] = norm_relu(zb[rows_at, 0:chan_m], 0).astype(BF16).reshape(per_chunk, half_w, chan_m)
                    start_pair(*u_copies(c))
                    return 0
                lax.fori_loop(0, CHUNKS, renorm_u, 0)
                clear_moments()

                def mid_body(c, _):
                    wait_halo(u_copies, c)
                    rows_at = pl.ds(pl.multiple_of(c * m_rows, m_rows), m_rows)
                    sl = pl.ds(c * per_chunk, per_chunk)
                    x = jnp.concatenate([u[r, sl].reshape(m_rows, chan_m) for r in range(3)], axis=1)
                    z = dot(x, wmid[j, :, chan_m:2 * chan_m])
                    z = z + from_left(dot(x, wmid[j, :, 0:chan_m]), half_w)
                    z = z + from_right(dot(x, wmid[j, :, 2 * chan_m:3 * chan_m]), half_w)
                    zb[rows_at, 0:chan_m] = z
                    add_moments(z, 0)
                    return 0
                lax.fori_loop(0, CHUNKS, mid_body, 0)
                send_moments(ar_mid + j, 0, chan_m)
                wait_sends(u_copies)
                recv_moments(ar_mid + j, bn_mid[j], 0, chan_m, count_b)

                clear_moments()
                for t in range(tiles):
                    cols = slice(t * TILE, (t + 1) * TILE)

                    def out_body(c, _):
                        rows_at = pl.ds(pl.multiple_of(c * m_rows, m_rows), m_rows)
                        if t == 0:
                            u2[rows_at, :] = norm_relu(zb[rows_at, 0:chan_m], 0).astype(BF16)
                        z = dot(u2[rows_at, :], wout[j, :, cols])
                        zb[rows_at, cols] = z
                        add_moments(z, t * TILE)
                        return 0
                    lax.fori_loop(0, CHUNKS, out_body, 0)
                    send_moments(ar_out + j * tiles + t, t * TILE, TILE)
                for t in range(tiles):
                    cols = slice(t * TILE, (t + 1) * TILE)
                    recv_moments(ar_out + j * tiles + t, bn_out[j, :, cols], t * TILE, TILE, count_b)

                    def next_h(c, _):
                        rows_at = pl.ds(pl.multiple_of(c * m_rows, m_rows), m_rows)
                        summed = norm(zb[rows_at, cols], t * TILE) + h[rows_at, cols].astype(F32)
                        h[rows_at, cols] = jnp.maximum(summed, 0.0).astype(BF16)
                        return 0
                    lax.fori_loop(0, CHUNKS, next_h, 0)
                return 0
            lax.fori_loop(0, blocks, block, 0)

            done = pltpu.make_async_copy(h, out, sem_out.at[0])
            done.start()
            done.wait()

        scratch = [
            pltpu.VMEM((4, batch, width, chan_a), BF16),
            pltpu.VMEM((3, batch, half_w, chan_m), BF16),
            pltpu.VMEM((points, chan_b), F32),
            pltpu.VMEM((points, chan_b), BF16),
            pltpu.VMEM((points, chan_m), BF16),
            pltpu.VMEM((layers, 3 * chan_a, 3 * chan_a), BF16),
            pltpu.VMEM((9 * chan_a, chan_b), BF16),
            pltpu.VMEM((blocks, chan_b, chan_m), BF16),
            pltpu.VMEM((blocks, 3 * chan_m, 3 * chan_m), BF16),
            pltpu.VMEM((blocks, chan_m, chan_b), BF16),
            pltpu.VMEM((2, 8, chan_b), F32),
            pltpu.VMEM((8, chan_b), F32),
            pltpu.VMEM((2, width, chan_a), F32),
            pltpu.VMEM((ar_total, 1, 2 * TILE), F32),
            pltpu.VMEM((ar_total, groups - 1, 1, 2 * TILE), F32),
            pltpu.SemaphoreType.DMA((5,)),
            pltpu.SemaphoreType.DMA((2, CHUNKS)),
            pltpu.SemaphoreType.DMA((2, CHUNKS)),
            pltpu.SemaphoreType.DMA((2, CHUNKS)),
            pltpu.SemaphoreType.DMA((2, CHUNKS)),
            pltpu.SemaphoreType.DMA((2, CHUNKS)),
            pltpu.SemaphoreType.DMA((ar_total,)),
            pltpu.SemaphoreType.DMA((ar_total,)),
            pltpu.SemaphoreType.DMA((1,)),
        ]
        return kernel, scratch, points

    def forward(images, w_a, bn_a, w_down, bn_down, w_in, bn_in, w_mid, bn_mid, w_out, bn_out):
        batch, rows, width, chan_a = images.shape
        chan_b, chan_m = w_in.shape[1:]
        kernel, scratch, points = make_kernel(batch, rows, width, chan_a, chan_b, chan_m, w_a.shape[0], w_in.shape[0])
        hbm = pl.BlockSpec(memory_space=pl.ANY)
        vmem = pl.BlockSpec(memory_space=pltpu.VMEM)
        res = pl.pallas_call(
            kernel,
            out_shape=jax.ShapeDtypeStruct((points, chan_b), BF16),
            in_specs=[hbm] * 6 + [vmem] * 5,
            out_specs=hbm,
            scratch_shapes=scratch,
            name="conv_stack",
            compiler_params=pltpu.CompilerParams(collective_id=0, has_side_effects=True, vmem_limit_bytes=67043328),
        )(images, w_a, w_down, w_in, w_mid, w_out, bn_a, bn_down, bn_in, bn_mid, bn_out)
        return res.reshape(batch, rows // 2, width // 2, chan_b)

    act_spec = P("dp", "sp", None, None)
    return jax.shard_map(forward, mesh=mesh, in_specs=(act_spec,) + (P(),) * 10, out_specs=act_spec, check_vma=False)
```

```python
import jax
import jax.numpy as jnp
from jax import lax
from jax.experimental import pallas as pl
from jax.experimental.pallas import tpu as pltpu
from jax.sharding import PartitionSpec as P

NORM_EPS = 1e-5
CHUNKS = 16
ROW_STEPS = 8
IN_STEPS = 4
OUT_STEPS = 2
TILE = 256
F32 = jnp.float32
BF16 = jnp.bfloat16


def solution(mesh):
    groups = mesh.shape["sp"]
    peers = sorted(range(1, groups), key=lambda k: (abs(2 * k - groups), k))

    def make_kernel(batch, rows, width, chan_a, chan_b, chan_m, layers, blocks):
        half_w = width // 2
        points = batch * half_w
        per_chunk = batch // CHUNKS
        half_b = batch // 2
        tiles = chan_b // TILE
        m_rows = points // CHUNKS
        pair_a = 2 * chan_a
        count_a = float(batch * rows * width * groups)
        count_b = float(points * groups)
        ar_in = layers
        ar_mid = ar_in + blocks
        ar_out = ar_mid + blocks
        ar_total = ar_out + (blocks + 1) * tiles

        def kernel(images, w_a, w_down, w_in, w_mid, w_out, bn_a, bn_down, bn_in, bn_mid, bn_out, h_out, u2_out, nrm_out,
                   xa, u, zb, h, u2, wa, wd, win, wmid, wout, st, nrm, prm, tmp, arsend, arbuf,
                   sem_w, sem_img, a_send, a_recv, u_send, u_recv, ar_ssem, ar_rsem, sem_out):
            me = lax.axis_index("sp")
            has_prev = me > 0
            has_next = me < groups - 1
            prev = jnp.maximum(me - 1, 0)
            nxt = jnp.minimum(me + 1, groups - 1)

            def remote(src, dst, ssem, rsem, dev):
                return pltpu.make_async_remote_copy(src_ref=src, dst_ref=dst, send_sem=ssem, recv_sem=rsem,
                                                    device_id={"sp": dev}, device_id_type=pl.DeviceIdType.MESH)

            def img_copy(c, r):
                sl = pl.ds(c * per_chunk, per_chunk)
                return pltpu.make_async_copy(images.at[sl, r], xa.at[1 + r, sl], sem_img.at[r, c])

            def load_images(c, _):
                for r in range(2):
                    img_copy(c, r).start()
                return 0
            lax.fori_loop(0, CHUNKS, load_images, 0)

            def wa_copies(start):
                for l in range(layers):
                    for dx in range(3):
                        for r in range(2):
                            for dy in range(3):
                                part = wa.at[l, pl.ds((r + dy) * chan_a, chan_a), pl.ds((2 * dx + r) * chan_a, chan_a)]
                                copy = pltpu.make_async_copy(w_a.at[l, dy, dx], part, sem_w.at[0])
                                if start:
                                    copy.start()
                                else:
                                    copy.wait()
            wa_copies(True)

            for l in range(layers):
                for dx in range(3):
                    for r in range(2):
                        wa[l, 3 * (1 - r) * chan_a:(3 * (1 - r) + 1) * chan_a, (2 * dx + r) * chan_a:(2 * dx + r + 1) * chan_a] = jnp.zeros((chan_a, chan_a), BF16)
            nrm[...] = jnp.zeros_like(nrm)
            prm[0] = bn_down[...]
            for j in range(blocks):
                prm[j + 1] = bn_out[j]

            barrier = pltpu.get_barrier_semaphore()
            for k in peers:
                pl.semaphore_signal(barrier, inc=1, device_id={"sp": lax.rem(me + k, groups)}, device_id_type=pl.DeviceIdType.MESH)
            pl.semaphore_wait(barrier, groups - 1)

            def a_copies(c, first):
                sl = pl.ds(c * per_chunk, per_chunk)
                top = images.at[sl, 0] if first else xa.at[1, sl]
                bot = images.at[sl, 1] if first else xa.at[2, sl]
                up = remote(top, xa.at[3, sl], a_send.at[0, c], a_recv.at[1, c], prev)
                down = remote(bot, xa.at[0, sl], a_send.at[1, c], a_recv.at[0, c], nxt)
                return up, down

            def d_copy(c):
                sl = pl.ds(c * per_chunk, per_chunk)
                return remote(u.at[0, sl], u.at[2, sl], u_send.at[0, c], u_recv.at[1, c], prev)

            def u_copies(c):
                sl = pl.ds(c * per_chunk, per_chunk)
                up = remote(u.at[1, sl], u.at[2, sl], u_send.at[0, c], u_recv.at[1, c], prev)
                down = remote(u.at[1, sl], u.at[0, sl], u_send.at[1, c], u_recv.at[0, c], nxt)
                return up, down

            def start_pair(up, down):
                @pl.when(has_prev)
                def _():
                    up.start()

                @pl.when(has_next)
                def _():
                    down.start()

            def wait_sends(pair_of):
                def body(c, _):
                    up, down = pair_of(c)

                    @pl.when(has_prev)
                    def _():
                        up.wait_send()

                    @pl.when(has_next)
                    def _():
                        down.wait_send()
                    return 0
                lax.fori_loop(0, CHUNKS, body, 0)

            def wait_halo(pair_of, c):
                up, down = pair_of(c)

                @pl.when(has_prev)
                def _():
                    down.wait_recv()

                @pl.when(has_next)
                def _():
                    up.wait_recv()

            def clear_moments():
                st[...] = jnp.zeros_like(st)

            def add_moments(z, lo):
                wide = z.shape[-1]
                z8 = z.reshape(z.shape[0] // 8, 8, wide)
                st[0, :, lo:lo + wide] += jnp.sum(z8, axis=0)
                st[1, :, lo:lo + wide] += jnp.sum(z8 * z8, axis=0)

            def ar_copy(a, k):
                return remote(arsend.at[a], arbuf.at[a, k - 1], ar_ssem.at[a], ar_rsem.at[a], lax.rem(me + k, groups))

            def pack_moments(a, lo):
                s = jnp.sum(st[0, :, lo:lo + TILE], axis=0, keepdims=True)
                q = jnp.sum(st[1, :, lo:lo + TILE], axis=0, keepdims=True)
                arsend[a] = jnp.concatenate([s, q], axis=1)

            def send_moments(a, lo):
                pack_moments(a, lo)
                for k in peers:
                    ar_copy(a, k).start()

            def ar_wait(a, sem):
                pltpu.make_async_copy(arbuf.at[a], arbuf.at[a], sem.at[a]).wait()

            def use_moments(a, params, lo, count):
                total = jnp.sum(arbuf[a], axis=0) + arsend[a]
                s = total[:, :TILE]
                q = total[:, TILE:]
                if count == count_a:
                    s = s[:, :chan_a] + s[:, chan_a:]
                    q = q[:, :chan_a] + q[:, chan_a:]
                m = s / count
                v = q / count - m * m
                scale = params[0:1] * lax.rsqrt(v + NORM_EPS)
                for at in range(lo, lo + TILE, m.shape[1]):
                    nrm[0:1, at:at + m.shape[1]] = m
                    nrm[1:2, at:at + m.shape[1]] = scale
                    nrm[2:3, at:at + m.shape[1]] = params[1:2]

            def recv_moments(a, params, lo, count):
                ar_wait(a, ar_rsem)
                use_moments(a, params, lo, count)
                ar_wait(a, ar_ssem)

            def tile_waits(j, t, sem):
                first = ar_out + j * tiles

                if t == 0:
                    @pl.when(j == 0)
                    def _():
                        every = arbuf.at[pl.ds(ar_out, tiles)]
                        pltpu.make_async_copy(every, every, sem.at[ar_out]).wait()

                @pl.when(j > 0)
                def _():
                    ar_wait(first + t, sem)

            def recv_tile(j, t):
                tile_waits(j, t, ar_rsem)
                use_moments(ar_out + j * tiles + t, prm[j, :, t * TILE:(t + 1) * TILE], t * TILE, count_b)
                tile_waits(j, t, ar_ssem)

            def norm(z, lo):
                wide = z.shape[-1]
                return (z - nrm[0:1, lo:lo + wide]) * nrm[1:2, lo:lo + wide] + nrm[2:3, lo:lo + wide]

            def norm_relu(z, lo):
                return jnp.maximum(norm(z, lo), 0.0)

            def from_left(y, wide):
                col = lax.broadcasted_iota(jnp.int32, y.shape, 0)
                return jnp.where(lax.rem(col, wide) == 0, 0.0, pltpu.roll(y, 1, 0))

            def from_right(y, wide):
                col = lax.broadcasted_iota(jnp.int32, y.shape, 0)
                return jnp.where(lax.rem(col, wide) == wide - 1, 0.0, pltpu.roll(y, y.shape[0] - 1, 0))

            def dot(x, w):
                return jnp.dot(x, w, preferred_element_type=F32)

            @pl.when(me == 0)
            def _():
                def body(b, _):
                    xa[0, b] = jnp.zeros((width, chan_a), BF16)
                    return 0
                lax.fori_loop(0, batch, body, 0)

            @pl.when(me == groups - 1)
            def _():
                def body(b, _):
                    xa[3, b] = jnp.zeros((width, chan_a), BF16)
                    u[2, b] = jnp.zeros((half_w, 2 * chan_a), BF16)
                    return 0
                lax.fori_loop(0, batch, body, 0)

            def send_a(c, _):
                start_pair(*a_copies(c, True))
                return 0
            lax.fori_loop(0, CHUNKS, send_a, 0)

            for dy in range(3):
                for dx in range(3):
                    row = (2 * dy + dx) * chan_a if dx < 2 else (6 + dy) * chan_a
                    pltpu.make_async_copy(w_down.at[dy, dx], wd.at[pl.ds(row, chan_a)], sem_w.at[1]).start()
                    for j in range(blocks):
                        pltpu.make_async_copy(w_mid.at[j, dy, dx], wmid.at[j, pl.ds(dy * chan_m, chan_m), pl.ds(dx * chan_m, chan_m)], sem_w.at[3]).start()
            pltpu.make_async_copy(w_in, win, sem_w.at[2]).start()
            pltpu.make_async_copy(w_out, wout, sem_w.at[4]).start()

            def wait_weight(ref, i):
                pltpu.make_async_copy(ref, ref, sem_w.at[i]).wait()

            wa_copies(False)

            def zero_h(c, _):
                h[pl.ds(pl.multiple_of(c * m_rows, m_rows), m_rows), :] = jnp.zeros((m_rows, chan_b), BF16)
                return 0
            lax.fori_loop(0, CHUNKS, zero_h, 0)

            def conv_a(l):
                clear_moments()
                for hb in range(2):
                    def body(i, _):
                        b = hb * half_b + i
                        c = b // per_chunk

                        @pl.when(lax.rem(b, per_chunk) == 0)
                        def _():
                            if l == 0:
                                for r in range(2):
                                    img_copy(c, r).wait()
                            wait_halo(lambda c: a_copies(c, l == 0), c)
                        x = jnp.concatenate([xa[r, b] for r in range(4)], axis=1)
                        z = dot(x, wa[l, :, pair_a:2 * pair_a])
                        z = z + from_left(dot(x, wa[l, :, 0:pair_a]), width)
                        z = z + from_right(dot(x, wa[l, :, 2 * pair_a:3 * pair_a]), width)
                        zb[pl.ds(pl.multiple_of(i * width, width), width), hb * pair_a:(hb + 1) * pair_a] = z
                        add_moments(z, 0)
                        return 0
                    lax.fori_loop(0, half_b, body, 0)
                send_moments(l, 0)
                wait_sends(lambda c: a_copies(c, l == 0))
                recv_moments(l, bn_a[l], 0, count_a)

            def normed_pair(hb, i):
                z = zb[pl.ds(pl.multiple_of(i * width, width), width), hb * pair_a:(hb + 1) * pair_a]
                return norm_relu(z, 0)

            conv_a(0)
            for l in range(1, layers):
                for hb in range(2):
                    def renorm(i, _):
                        b = hb * half_b + i
                        y = normed_pair(hb, i).astype(BF16)
                        xa[1, b] = y[:, :chan_a]
                        xa[2, b] = y[:, chan_a:]

                        @pl.when(lax.rem(b, per_chunk) == per_chunk - 1)
                        def _():
                            start_pair(*a_copies(b // per_chunk, False))
                        return 0
                    lax.fori_loop(0, half_b, renorm, 0)
                conv_a(l)

            for hb in range(2):
                def pair_up(i, _):
                    b = hb * half_b + i
                    y = normed_pair(hb, i)
                    for r in range(2):
                        tmp[r] = y[:, r * chan_a:(r + 1) * chan_a]
                        u[r, b, :, 0:chan_a] = tmp[r, pl.ds(0, half_w, stride=2), :].astype(BF16)
                        u[r, b, :, chan_a:2 * chan_a] = tmp[r, pl.ds(1, half_w, stride=2), :].astype(BF16)

                    @pl.when(jnp.logical_and(lax.rem(b, per_chunk) == per_chunk - 1, has_prev))
                    def _():
                        d_copy(b // per_chunk).start()
                    return 0
                lax.fori_loop(0, half_b, pair_up, 0)

            wait_weight(wd, 1)
            clear_moments()

            def down_body(c, _):
                @pl.when(has_next)
                def _():
                    d_copy(c).wait_recv()
                sl = pl.ds(c * per_chunk, per_chunk)
                flat = [u[r, sl].reshape(m_rows, 2 * chan_a) for r in range(3)]
                evens = [from_right(f[:, :chan_a].astype(F32), half_w).astype(BF16) for f in flat]
                x = jnp.concatenate(flat + evens, axis=1)
                rows_at = pl.ds(pl.multiple_of(c * m_rows, m_rows), m_rows)
                for t in range(tiles):
                    z = dot(x, wd[:, t * TILE:(t + 1) * TILE])
                    zb[rows_at, t * TILE:(t + 1) * TILE] = z
                    add_moments(z, t * TILE)
                return 0
            lax.fori_loop(0, CHUNKS, down_body, 0)
            for t in range(tiles):
                pack_moments(ar_out + t, t * TILE)
            every_tile = pl.ds(ar_out, tiles)
            for k in peers:
                remote(arsend.at[every_tile], arbuf.at[every_tile, k - 1], ar_ssem.at[ar_out], ar_rsem.at[ar_out], lax.rem(me + k, groups)).start()

            def wait_d(c, _):
                @pl.when(has_prev)
                def _():
                    d_copy(c).wait_send()
                return 0
            lax.fori_loop(0, CHUNKS, wait_d, 0)

            @pl.when(me == 0)
            def _():
                def body(b, _):
                    u[0, b] = jnp.zeros((half_w, chan_m), BF16)
                    return 0
                lax.fori_loop(0, batch, body, 0)

            wait_weight(win, 2)
            wait_weight(wmid, 3)
            wait_weight(wout, 4)

            def next_h(rows_at, t):
                cols = slice(t * TILE, (t + 1) * TILE)
                summed = norm(zb[rows_at, cols], t * TILE) + h[rows_at, cols].astype(F32)
                return jnp.maximum(summed, 0.0).astype(BF16)

            def h_copy():
                return pltpu.make_async_copy(h, h_out, sem_out.at[0])

            def u2_copy():
                return pltpu.make_async_copy(u2, u2_out, sem_out.at[1])

            def block(j, _):
                for t in range(tiles - 1):
                    recv_tile(j, t)

                    def tile_body(c, _):
                        rows_at = pl.ds(pl.multiple_of(c * (points // ROW_STEPS), points // ROW_STEPS), points // ROW_STEPS)
                        h[rows_at, t * TILE:(t + 1) * TILE] = next_h(rows_at, t)
                        return 0
                    lax.fori_loop(0, ROW_STEPS, tile_body, 0)
                recv_tile(j, tiles - 1)
                clear_moments()

                def in_body(c, _):
                    rows_at = pl.ds(pl.multiple_of(c * (points // IN_STEPS), points // IN_STEPS), points // IN_STEPS)
                    last = next_h(rows_at, tiles - 1)
                    h[rows_at, chan_b - TILE:chan_b] = last
                    z = dot(jnp.concatenate([h[rows_at, 0:chan_b - TILE], last], axis=1), win[j])
                    zb[rows_at, 0:chan_m] = z
                    add_moments(z, 0)
                    return 0
                lax.fori_loop(0, IN_STEPS, in_body, 0)
                send_moments(ar_in + j, 0)

                @pl.when(j == blocks - 1)
                def _():
                    h_copy().start()
                recv_moments(ar_in + j, bn_in[j], 0, count_b)

                def renorm_u(c, _):
                    rows_at = pl.ds(pl.multiple_of(c * m_rows, m_rows), m_rows)
                    sl = pl.ds(c * per_chunk, per_chunk)
                    u[1, sl] = norm_relu(zb[rows_at, 0:chan_m], 0).astype(BF16).reshape(per_chunk, half_w, chan_m)
                    start_pair(*u_copies(c))
                    return 0
                lax.fori_loop(0, CHUNKS, renorm_u, 0)
                clear_moments()

                def mid_body(c, _):
                    wait_halo(u_copies, c)
                    rows_at = pl.ds(pl.multiple_of(c * m_rows, m_rows), m_rows)
                    sl = pl.ds(c * per_chunk, per_chunk)
                    x = jnp.concatenate([u[r, sl].reshape(m_rows, chan_m) for r in range(3)], axis=1)
                    z = dot(x, wmid[j, :, chan_m:2 * chan_m])
                    z = z + from_left(dot(x, wmid[j, :, 0:chan_m]), half_w)
                    z = z + from_right(dot(x, wmid[j, :, 2 * chan_m:3 * chan_m]), half_w)
                    zb[rows_at, 0:chan_m] = z
                    add_moments(z, 0)
                    return 0
                lax.fori_loop(0, CHUNKS, mid_body, 0)
                send_moments(ar_mid + j, 0)
                wait_sends(u_copies)
                recv_moments(ar_mid + j, bn_mid[j], 0, count_b)

                clear_moments()
                for t in range(tiles):
                    cols = slice(t * TILE, (t + 1) * TILE)

                    def out_body(c, _):
                        rows_at = pl.ds(pl.multiple_of(c * (points // OUT_STEPS), points // OUT_STEPS), points // OUT_STEPS)
                        if t == 0:
                            u2[rows_at, :] = norm_relu(zb[rows_at, 0:chan_m], 0).astype(BF16)
                        z = dot(u2[rows_at, :], wout[j, :, cols])
                        zb[rows_at, cols] = z
                        add_moments(z, t * TILE)
                        return 0
                    lax.fori_loop(0, OUT_STEPS, out_body, 0)
                    send_moments(ar_out + (j + 1) * tiles + t, t * TILE)
                    if t == 0:
                        @pl.when(j == blocks - 1)
                        def _():
                            u2_copy().start()
                return 0
            lax.fori_loop(0, blocks, block, 0)

            for t in range(tiles):
                recv_tile(blocks, t)
            nrm_copy = pltpu.make_async_copy(nrm, nrm_out, sem_out.at[2])
            nrm_copy.start()
            h_copy().wait()
            u2_copy().wait()
            nrm_copy.wait()

        scratch = [
            pltpu.VMEM((4, batch, width, chan_a), BF16),
            pltpu.VMEM((3, batch, half_w, chan_m), BF16),
            pltpu.VMEM((points, chan_b), F32),
            pltpu.VMEM((points, chan_b), BF16),
            pltpu.VMEM((points, chan_m), BF16),
            pltpu.VMEM((layers, 4 * chan_a, 6 * chan_a), BF16),
            pltpu.VMEM((9 * chan_a, chan_b), BF16),
            pltpu.VMEM((blocks, chan_b, chan_m), BF16),
            pltpu.VMEM((blocks, 3 * chan_m, 3 * chan_m), BF16),
            pltpu.VMEM((blocks, chan_m, chan_b), BF16),
            pltpu.VMEM((2, 8, chan_b), F32),
            pltpu.VMEM((8, chan_b), F32),
            pltpu.VMEM((blocks + 1, 2, chan_b), F32),
            pltpu.VMEM((2, width, chan_a), F32),
            pltpu.VMEM((ar_total, 1, 2 * TILE), F32),
            pltpu.VMEM((ar_total, groups - 1, 1, 2 * TILE), F32),
            pltpu.SemaphoreType.DMA((5,)),
            pltpu.SemaphoreType.DMA((2, CHUNKS)),
            pltpu.SemaphoreType.DMA((2, CHUNKS)),
            pltpu.SemaphoreType.DMA((2, CHUNKS)),
            pltpu.SemaphoreType.DMA((2, CHUNKS)),
            pltpu.SemaphoreType.DMA((2, CHUNKS)),
            pltpu.SemaphoreType.DMA((ar_total,)),
            pltpu.SemaphoreType.DMA((ar_total,)),
            pltpu.SemaphoreType.DMA((3,)),
        ]
        return kernel, scratch, points

    def forward(images, w_a, bn_a, w_down, bn_down, w_in, bn_in, w_mid, bn_mid, w_out, bn_out):
        batch, rows, width, chan_a = images.shape
        chan_b, chan_m = w_in.shape[1:]
        kernel, scratch, points = make_kernel(batch, rows, width, chan_a, chan_b, chan_m, w_a.shape[0], w_in.shape[0])
        hbm = pl.BlockSpec(memory_space=pl.ANY)
        vmem = pl.BlockSpec(memory_space=pltpu.VMEM)
        h_last, branch, moments = pl.pallas_call(
            kernel,
            out_shape=(jax.ShapeDtypeStruct((points, chan_b), BF16),
                       jax.ShapeDtypeStruct((points, chan_m), BF16),
                       jax.ShapeDtypeStruct((8, chan_b), F32)),
            in_specs=[hbm] * 6 + [vmem] * 5,
            out_specs=(hbm, hbm, hbm),
            scratch_shapes=scratch,
            name="conv_stack",
            compiler_params=pltpu.CompilerParams(collective_id=0, has_side_effects=True, vmem_limit_bytes=67043328),
        )(images, w_a, w_down, w_in, w_mid, w_out, bn_a, bn_down, bn_in, bn_mid, bn_out)

        step = points // ROW_STEPS
        last = w_out.shape[0] - 1

        def finish(branch_ref, h_ref, w_ref, nrm_ref, out_ref):
            for t in range(chan_b // TILE):
                cols = slice(t * TILE, (t + 1) * TILE)
                z = jnp.dot(branch_ref[...], w_ref[0, :, cols], preferred_element_type=F32)
                normed = (z - nrm_ref[0:1, cols]) * nrm_ref[1:2, cols] + nrm_ref[2:3, cols]
                out_ref[:, cols] = jnp.maximum(normed + h_ref[:, cols].astype(F32), 0.0).astype(BF16)

        res = pl.pallas_call(
            finish,
            grid=(ROW_STEPS,),
            out_shape=jax.ShapeDtypeStruct((points, chan_b), BF16),
            in_specs=[pl.BlockSpec((step, chan_m), lambda i: (i, 0)),
                      pl.BlockSpec((step, chan_b), lambda i: (i, 0)),
                      pl.BlockSpec((1, chan_m, chan_b), lambda i: (last, 0, 0)),
                      pl.BlockSpec((8, chan_b), lambda i: (0, 0))],
            out_specs=pl.BlockSpec((step, chan_b), lambda i: (i, 0)),
            name="last_norm",
        )(branch, h_last, w_out, moments)
        return res.reshape(batch, rows // 2, width // 2, chan_b)

    act_spec = P("dp", "sp", None, None)
    return jax.shard_map(forward, mesh=mesh, in_specs=(act_spec,) + (P(),) * 10, out_specs=act_spec, check_vma=False)
```

```python
import jax
import jax.numpy as jnp
from jax import lax
from jax.experimental import pallas as pl
from jax.experimental.pallas import tpu as pltpu
from jax.sharding import PartitionSpec as P

NORM_EPS = 1e-5
CHUNKS = 16
ROW_STEPS = 8
IN_STEPS = 4
OUT_STEPS = 2
LAST_STEPS = 4
EARLY_A = 4
EARLY_B = 4
TILE = 256
F32 = jnp.float32
BF16 = jnp.bfloat16


def solution(mesh):
    groups = mesh.shape["sp"]
    peers = sorted(range(1, groups), key=lambda k: (abs(2 * k - groups), k))

    def make_kernel(batch, rows, width, chan_a, chan_b, chan_m, layers, blocks):
        half_w = width // 2
        points = batch * half_w
        per_chunk = batch // CHUNKS
        half_b = batch // 2
        tiles = chan_b // TILE
        m_rows = points // CHUNKS
        pair_a = 2 * chan_a
        early_a = EARLY_A // per_chunk
        early_b = EARLY_B // per_chunk
        count_a = float(batch * rows * width * groups)
        count_b = float(points * groups)
        ar_in = layers
        ar_mid = ar_in + blocks
        ar_out = ar_mid + blocks
        ar_total = ar_out + (blocks + 1) * tiles

        def kernel(images, w_a, w_down, w_in, w_mid, w_out, bn_a, bn_down, bn_in, bn_mid, bn_out, h_out, u2_out, nrm_out,
                   xa, u, zb, h, u2, wa, wd, win, wmid, wout, st, nrm, prm, tmp, arsend, arbuf, ez_a, ez_d, ez_b,
                   sem_w, sem_img, a_send, a_recv, u_send, u_recv, ar_ssem, ar_rsem, e_send, e_recv, sem_out):
            me = lax.axis_index("sp")
            has_prev = me > 0
            has_next = me < groups - 1
            prev = jnp.maximum(me - 1, 0)
            nxt = jnp.minimum(me + 1, groups - 1)

            def remote(src, dst, ssem, rsem, dev):
                return pltpu.make_async_remote_copy(src_ref=src, dst_ref=dst, send_sem=ssem, recv_sem=rsem,
                                                    device_id={"sp": dev}, device_id_type=pl.DeviceIdType.MESH)

            def img_copy(c, r):
                sl = pl.ds(c * per_chunk, per_chunk)
                return pltpu.make_async_copy(images.at[sl, r], xa.at[1 + r, sl], sem_img.at[r, c])

            def load_images(c, _):
                for r in range(2):
                    img_copy(c, r).start()
                return 0
            lax.fori_loop(0, CHUNKS, load_images, 0)

            def wa_copies(start):
                for l in range(layers):
                    for dx in range(3):
                        for r in range(2):
                            for dy in range(3):
                                part = wa.at[l, pl.ds((r + dy) * chan_a, chan_a), pl.ds((2 * dx + r) * chan_a, chan_a)]
                                copy = pltpu.make_async_copy(w_a.at[l, dy, dx], part, sem_w.at[0])
                                if start:
                                    copy.start()
                                else:
                                    copy.wait()
            wa_copies(True)

            for l in range(layers):
                for dx in range(3):
                    for r in range(2):
                        wa[l, 3 * (1 - r) * chan_a:(3 * (1 - r) + 1) * chan_a, (2 * dx + r) * chan_a:(2 * dx + r + 1) * chan_a] = jnp.zeros((chan_a, chan_a), BF16)
            nrm[...] = jnp.zeros_like(nrm)
            prm[0] = bn_down[...]
            for j in range(blocks):
                prm[j + 1] = bn_out[j]

            barrier = pltpu.get_barrier_semaphore()
            for k in peers:
                pl.semaphore_signal(barrier, inc=1, device_id={"sp": lax.rem(me + k, groups)}, device_id_type=pl.DeviceIdType.MESH)
            pl.semaphore_wait(barrier, groups - 1)

            def a_copies(c, first):
                sl = pl.ds(c * per_chunk, per_chunk)
                top = images.at[sl, 0] if first else xa.at[1, sl]
                bot = images.at[sl, 1] if first else xa.at[2, sl]
                up = remote(top, xa.at[3, sl], a_send.at[0, c], a_recv.at[1, c], prev)
                down = remote(bot, xa.at[0, sl], a_send.at[1, c], a_recv.at[0, c], nxt)
                return up, down

            def d_copy(c):
                sl = pl.ds(c * per_chunk, per_chunk)
                return remote(u.at[0, sl], u.at[2, sl], u_send.at[0, c], u_recv.at[1, c], prev)

            def u_copies(c):
                sl = pl.ds(c * per_chunk, per_chunk)
                up = remote(u.at[1, sl], u.at[2, sl], u_send.at[0, c], u_recv.at[1, c], prev)
                down = remote(u.at[1, sl], u.at[0, sl], u_send.at[1, c], u_recv.at[0, c], nxt)
                return up, down

            def start_pair(up, down):
                @pl.when(has_prev)
                def _():
                    up.start()

                @pl.when(has_next)
                def _():
                    down.start()

            def wait_sends(pair_of, first=0):
                def body(c, _):
                    up, down = pair_of(c)

                    @pl.when(has_prev)
                    def _():
                        up.wait_send()

                    @pl.when(has_next)
                    def _():
                        down.wait_send()
                    return 0
                lax.fori_loop(first, CHUNKS, body, 0)

            def early_a_copies(l):
                rows_at = pl.ds(0, EARLY_A * width)
                if l == layers - 1:
                    return remote(zb.at[rows_at, pl.ds(0, chan_a)], ez_d, e_send.at[l, 0], e_recv.at[l, 1], prev), None
                up = remote(zb.at[rows_at, pl.ds(0, chan_a)], ez_a.at[l, 1], e_send.at[l, 0], e_recv.at[l, 1], prev)
                down = remote(zb.at[rows_at, pl.ds(chan_a, chan_a)], ez_a.at[l, 0], e_send.at[l, 1], e_recv.at[l, 0], nxt)
                return up, down

            def early_b_copies():
                src = zb.at[pl.ds(0, EARLY_B * half_w), pl.ds(0, chan_m)]
                up = remote(src, ez_b.at[1], e_send.at[layers, 0], e_recv.at[layers, 1], prev)
                down = remote(src, ez_b.at[0], e_send.at[layers, 1], e_recv.at[layers, 0], nxt)
                return up, down

            def start_early(up, down):
                @pl.when(has_prev)
                def _():
                    up.start()
                if down is not None:
                    @pl.when(has_next)
                    def _():
                        down.start()

            def sent_early(up, down):
                @pl.when(has_prev)
                def _():
                    up.wait_send()
                if down is not None:
                    @pl.when(has_next)
                    def _():
                        down.wait_send()

            def take_early(up, down, from_prev, from_next, count):
                if down is not None:
                    @pl.when(has_prev)
                    def _():
                        down.wait_recv()
                        lax.fori_loop(0, count, from_prev, 0)

                @pl.when(has_next)
                def _():
                    up.wait_recv()
                    lax.fori_loop(0, count, from_next, 0)

            def wait_halo(pair_of, c):
                up, down = pair_of(c)

                @pl.when(has_prev)
                def _():
                    down.wait_recv()

                @pl.when(has_next)
                def _():
                    up.wait_recv()

            def clear_moments():
                st[...] = jnp.zeros_like(st)

            def add_moments(z, lo):
                wide = z.shape[-1]
                part = min(512, z.shape[0])
                for p in range(0, z.shape[0], part):
                    z8 = z[p:p + part].reshape(part // 8, 8, wide)
                    st[0, :, lo:lo + wide] += jnp.sum(z8, axis=0)
                    st[1, :, lo:lo + wide] += jnp.sum(z8 * z8, axis=0)

            def ar_copy(a, k):
                return remote(arsend.at[a], arbuf.at[a, k - 1], ar_ssem.at[a], ar_rsem.at[a], lax.rem(me + k, groups))

            def pack_moments(a, lo):
                s = jnp.sum(st[0, :, lo:lo + TILE], axis=0, keepdims=True)
                q = jnp.sum(st[1, :, lo:lo + TILE], axis=0, keepdims=True)
                arsend[a] = jnp.concatenate([s, q], axis=1)

            def send_moments(a, lo):
                pack_moments(a, lo)
                for k in peers:
                    ar_copy(a, k).start()

            def ar_wait(a, sem):
                pltpu.make_async_copy(arbuf.at[a], arbuf.at[a], sem.at[a]).wait()

            def use_moments(a, params, lo, count):
                total = jnp.sum(arbuf[a], axis=0) + arsend[a]
                s = total[:, :TILE]
                q = total[:, TILE:]
                if count == count_a:
                    s = s[:, :chan_a] + s[:, chan_a:]
                    q = q[:, :chan_a] + q[:, chan_a:]
                m = s / count
                v = q / count - m * m
                scale = params[0:1] * lax.rsqrt(v + NORM_EPS)
                for at in range(lo, lo + TILE, m.shape[1]):
                    nrm[0:1, at:at + m.shape[1]] = m
                    nrm[1:2, at:at + m.shape[1]] = scale
                    nrm[2:3, at:at + m.shape[1]] = params[1:2]

            def recv_moments(a, params, lo, count):
                ar_wait(a, ar_rsem)
                use_moments(a, params, lo, count)
                ar_wait(a, ar_ssem)

            def tile_waits(j, t, sem):
                first = ar_out + j * tiles

                if t == 0:
                    @pl.when(j == 0)
                    def _():
                        every = arbuf.at[pl.ds(ar_out, tiles)]
                        pltpu.make_async_copy(every, every, sem.at[ar_out]).wait()

                @pl.when(j > 0)
                def _():
                    ar_wait(first + t, sem)

            def recv_tile(j, t):
                tile_waits(j, t, ar_rsem)
                use_moments(ar_out + j * tiles + t, prm[j, :, t * TILE:(t + 1) * TILE], t * TILE, count_b)
                tile_waits(j, t, ar_ssem)

            def norm(z, lo):
                wide = z.shape[-1]
                return (z - nrm[0:1, lo:lo + wide]) * nrm[1:2, lo:lo + wide] + nrm[2:3, lo:lo + wide]

            def norm_relu(z, lo):
                return jnp.maximum(norm(z, lo), 0.0)

            def from_left(y, wide):
                col = lax.broadcasted_iota(jnp.int32, y.shape, 0)
                return jnp.where(lax.rem(col, wide) == 0, 0.0, pltpu.roll(y, 1, 0))

            def from_right(y, wide):
                col = lax.broadcasted_iota(jnp.int32, y.shape, 0)
                return jnp.where(lax.rem(col, wide) == wide - 1, 0.0, pltpu.roll(y, y.shape[0] - 1, 0))

            def dot(x, w):
                return jnp.dot(x, w, preferred_element_type=F32)

            @pl.when(me == 0)
            def _():
                def body(b, _):
                    xa[0, b] = jnp.zeros((width, chan_a), BF16)
                    return 0
                lax.fori_loop(0, batch, body, 0)

            @pl.when(me == groups - 1)
            def _():
                def body(b, _):
                    xa[3, b] = jnp.zeros((width, chan_a), BF16)
                    u[2, b] = jnp.zeros((half_w, 2 * chan_a), BF16)
                    return 0
                lax.fori_loop(0, batch, body, 0)

            def send_a(c, _):
                start_pair(*a_copies(c, True))
                return 0
            lax.fori_loop(0, CHUNKS, send_a, 0)

            for dy in range(3):
                for dx in range(3):
                    row = (2 * dy + dx) * chan_a if dx < 2 else (6 + dy) * chan_a
                    pltpu.make_async_copy(w_down.at[dy, dx], wd.at[pl.ds(row, chan_a)], sem_w.at[1]).start()
                    for j in range(blocks):
                        pltpu.make_async_copy(w_mid.at[j, dy, dx], wmid.at[j, pl.ds(dy * chan_m, chan_m), pl.ds(dx * chan_m, chan_m)], sem_w.at[3]).start()
            pltpu.make_async_copy(w_in, win, sem_w.at[2]).start()
            pltpu.make_async_copy(w_out, wout, sem_w.at[4]).start()

            def wait_weight(ref, i):
                pltpu.make_async_copy(ref, ref, sem_w.at[i]).wait()

            wa_copies(False)

            def zero_h(c, _):
                h[pl.ds(pl.multiple_of(c * m_rows, m_rows), m_rows), :] = jnp.zeros((m_rows, chan_b), BF16)
                return 0
            lax.fori_loop(0, CHUNKS, zero_h, 0)

            def conv_a(l):
                clear_moments()
                for hb in range(2):
                    def body(i, _):
                        b = hb * half_b + i
                        c = b // per_chunk

                        @pl.when(jnp.logical_and(lax.rem(b, per_chunk) == 0, c >= (early_a if l else 0)))
                        def _():
                            if l == 0:
                                for r in range(2):
                                    img_copy(c, r).wait()
                            wait_halo(lambda c: a_copies(c, l == 0), c)
                        x = jnp.concatenate([xa[r, b] for r in range(4)], axis=1)
                        z = dot(x, wa[l, :, pair_a:2 * pair_a])
                        z = z + from_left(dot(x, wa[l, :, 0:pair_a]), width)
                        z = z + from_right(dot(x, wa[l, :, 2 * pair_a:3 * pair_a]), width)
                        zb[pl.ds(pl.multiple_of(i * width, width), width), hb * pair_a:(hb + 1) * pair_a] = z
                        add_moments(z, 0)
                        return 0
                    lax.fori_loop(0, half_b, body, 0)
                send_moments(l, 0)
                start_early(*early_a_copies(l))
                wait_sends(lambda c: a_copies(c, l == 0), early_a if l else 0)
                recv_moments(l, bn_a[l], 0, count_a)

            def normed_pair(hb, i):
                z = zb[pl.ds(pl.multiple_of(i * width, width), width), hb * pair_a:(hb + 1) * pair_a]
                return norm_relu(z, 0)

            conv_a(0)
            for l in range(1, layers):
                for hb in range(2):
                    def renorm(i, _):
                        b = hb * half_b + i
                        y = normed_pair(hb, i).astype(BF16)
                        xa[1, b] = y[:, :chan_a]
                        xa[2, b] = y[:, chan_a:]

                        @pl.when(jnp.logical_and(lax.rem(b, per_chunk) == per_chunk - 1, b >= EARLY_A))
                        def _():
                            start_pair(*a_copies(b // per_chunk, False))
                        return 0
                    lax.fori_loop(0, half_b, renorm, 0)

                def early_rows(side, slot):
                    def body(b, _):
                        z = ez_a[l - 1, side, pl.ds(pl.multiple_of(b * width, width), width), :]
                        xa[slot, b] = norm_relu(z, 0).astype(BF16)
                        return 0
                    return body
                up, down = early_a_copies(l - 1)
                take_early(up, down, early_rows(0, 0), early_rows(1, 3), EARLY_A)
                sent_early(up, down)
                conv_a(l)

            for hb in range(2):
                def pair_up(i, _):
                    b = hb * half_b + i
                    y = normed_pair(hb, i)
                    for r in range(2):
                        tmp[r] = y[:, r * chan_a:(r + 1) * chan_a]
                        u[r, b, :, 0:chan_a] = tmp[r, pl.ds(0, half_w, stride=2), :].astype(BF16)
                        u[r, b, :, chan_a:2 * chan_a] = tmp[r, pl.ds(1, half_w, stride=2), :].astype(BF16)

                    @pl.when(jnp.logical_and(jnp.logical_and(lax.rem(b, per_chunk) == per_chunk - 1, b >= EARLY_A), has_prev))
                    def _():
                        d_copy(b // per_chunk).start()
                    return 0
                lax.fori_loop(0, half_b, pair_up, 0)

            def early_pair(b, _):
                tmp[0] = norm_relu(ez_d[pl.ds(pl.multiple_of(b * width, width), width), :], 0)
                u[2, b, :, 0:chan_a] = tmp[0, pl.ds(0, half_w, stride=2), :].astype(BF16)
                u[2, b, :, chan_a:2 * chan_a] = tmp[0, pl.ds(1, half_w, stride=2), :].astype(BF16)
                return 0
            up, down = early_a_copies(layers - 1)
            take_early(up, down, None, early_pair, EARLY_A)
            sent_early(up, down)
            wait_weight(wd, 1)
            clear_moments()

            def down_body(c, _):
                @pl.when(jnp.logical_and(has_next, c >= early_a))
                def _():
                    d_copy(c).wait_recv()
                sl = pl.ds(c * per_chunk, per_chunk)
                flat = [u[r, sl].reshape(m_rows, 2 * chan_a) for r in range(3)]
                evens = [from_right(f[:, :chan_a].astype(F32), half_w).astype(BF16) for f in flat]
                x = jnp.concatenate(flat + evens, axis=1)
                rows_at = pl.ds(pl.multiple_of(c * m_rows, m_rows), m_rows)
                for t in range(tiles):
                    z = dot(x, wd[:, t * TILE:(t + 1) * TILE])
                    zb[rows_at, t * TILE:(t + 1) * TILE] = z
                    add_moments(z, t * TILE)
                return 0
            lax.fori_loop(0, CHUNKS, down_body, 0)
            for t in range(tiles):
                pack_moments(ar_out + t, t * TILE)
            every_tile = pl.ds(ar_out, tiles)
            for k in peers:
                remote(arsend.at[every_tile], arbuf.at[every_tile, k - 1], ar_ssem.at[ar_out], ar_rsem.at[ar_out], lax.rem(me + k, groups)).start()

            def wait_d(c, _):
                @pl.when(has_prev)
                def _():
                    d_copy(c).wait_send()
                return 0
            lax.fori_loop(early_a, CHUNKS, wait_d, 0)

            @pl.when(me == 0)
            def _():
                def body(b, _):
                    u[0, b] = jnp.zeros((half_w, chan_m), BF16)
                    return 0
                lax.fori_loop(0, batch, body, 0)

            wait_weight(win, 2)
            wait_weight(wmid, 3)
            wait_weight(wout, 4)

            def next_h(rows_at, t):
                cols = slice(t * TILE, (t + 1) * TILE)
                summed = norm(zb[rows_at, cols], t * TILE) + h[rows_at, cols].astype(F32)
                return jnp.maximum(summed, 0.0).astype(BF16)

            def h_copy():
                return pltpu.make_async_copy(h, h_out, sem_out.at[0])

            def u2_copy():
                return pltpu.make_async_copy(u2, u2_out, sem_out.at[1])

            def block(j, _):
                for t in range(tiles - 1):
                    recv_tile(j, t)

                    def tile_body(c, _):
                        rows_at = pl.ds(pl.multiple_of(c * (points // ROW_STEPS), points // ROW_STEPS), points // ROW_STEPS)
                        h[rows_at, t * TILE:(t + 1) * TILE] = next_h(rows_at, t)
                        return 0
                    lax.fori_loop(0, ROW_STEPS, tile_body, 0)
                recv_tile(j, tiles - 1)
                clear_moments()

                def in_body(c, _):
                    rows_at = pl.ds(pl.multiple_of(c * (points // IN_STEPS), points // IN_STEPS), points // IN_STEPS)
                    last = next_h(rows_at, tiles - 1)
                    h[rows_at, chan_b - TILE:chan_b] = last
                    z = dot(jnp.concatenate([h[rows_at, 0:chan_b - TILE], last], axis=1), win[j])
                    zb[rows_at, 0:chan_m] = z
                    add_moments(z, 0)
                    return 0
                lax.fori_loop(0, IN_STEPS, in_body, 0)
                send_moments(ar_in + j, 0)
                start_early(*early_b_copies())

                @pl.when(j == blocks - 1)
                def _():
                    h_copy().start()
                recv_moments(ar_in + j, bn_in[j], 0, count_b)

                def renorm_u(c, _):
                    rows_at = pl.ds(pl.multiple_of(c * m_rows, m_rows), m_rows)
                    sl = pl.ds(c * per_chunk, per_chunk)
                    u[1, sl] = norm_relu(zb[rows_at, 0:chan_m], 0).astype(BF16).reshape(per_chunk, half_w, chan_m)

                    @pl.when(c >= early_b)
                    def _():
                        start_pair(*u_copies(c))
                    return 0
                lax.fori_loop(0, CHUNKS, renorm_u, 0)

                def early_u(side, slot):
                    def body(b, _):
                        z = ez_b[side, pl.ds(pl.multiple_of(b * half_w, half_w), half_w), :]
                        u[slot, b] = norm_relu(z, 0).astype(BF16)
                        return 0
                    return body
                up, down = early_b_copies()
                take_early(up, down, early_u(0, 0), early_u(1, 2), EARLY_B)
                sent_early(up, down)
                clear_moments()

                def mid_body(c, _):
                    @pl.when(c >= early_b)
                    def _():
                        wait_halo(u_copies, c)
                    rows_at = pl.ds(pl.multiple_of(c * m_rows, m_rows), m_rows)
                    sl = pl.ds(c * per_chunk, per_chunk)
                    x = jnp.concatenate([u[r, sl].reshape(m_rows, chan_m) for r in range(3)], axis=1)
                    z = dot(x, wmid[j, :, chan_m:2 * chan_m])
                    z = z + from_left(dot(x, wmid[j, :, 0:chan_m]), half_w)
                    z = z + from_right(dot(x, wmid[j, :, 2 * chan_m:3 * chan_m]), half_w)
                    zb[rows_at, 0:chan_m] = z
                    add_moments(z, 0)
                    return 0
                lax.fori_loop(0, CHUNKS, mid_body, 0)
                send_moments(ar_mid + j, 0)
                wait_sends(u_copies, early_b)
                recv_moments(ar_mid + j, bn_mid[j], 0, count_b)

                clear_moments()
                for t in range(tiles):
                    cols = slice(t * TILE, (t + 1) * TILE)

                    def out_body(c, _):
                        rows_at = pl.ds(pl.multiple_of(c * (points // OUT_STEPS), points // OUT_STEPS), points // OUT_STEPS)
                        if t == 0:
                            u2[rows_at, :] = norm_relu(zb[rows_at, 0:chan_m], 0).astype(BF16)
                        z = dot(u2[rows_at, :], wout[j, :, cols])
                        zb[rows_at, cols] = z
                        add_moments(z, t * TILE)
                        return 0
                    lax.fori_loop(0, OUT_STEPS, out_body, 0)
                    send_moments(ar_out + (j + 1) * tiles + t, t * TILE)
                    if t == 0:
                        @pl.when(j == blocks - 1)
                        def _():
                            u2_copy().start()
                return 0
            lax.fori_loop(0, blocks, block, 0)

            for t in range(tiles):
                recv_tile(blocks, t)
            nrm_copy = pltpu.make_async_copy(nrm, nrm_out, sem_out.at[2])
            nrm_copy.start()
            h_copy().wait()
            u2_copy().wait()
            nrm_copy.wait()

        scratch = [
            pltpu.VMEM((4, batch, width, chan_a), BF16),
            pltpu.VMEM((3, batch, half_w, chan_m), BF16),
            pltpu.VMEM((points, chan_b), F32),
            pltpu.VMEM((points, chan_b), BF16),
            pltpu.VMEM((points, chan_m), BF16),
            pltpu.VMEM((layers, 4 * chan_a, 6 * chan_a), BF16),
            pltpu.VMEM((9 * chan_a, chan_b), BF16),
            pltpu.VMEM((blocks, chan_b, chan_m), BF16),
            pltpu.VMEM((blocks, 3 * chan_m, 3 * chan_m), BF16),
            pltpu.VMEM((blocks, chan_m, chan_b), BF16),
            pltpu.VMEM((2, 8, chan_b), F32),
            pltpu.VMEM((8, chan_b), F32),
            pltpu.VMEM((blocks + 1, 2, chan_b), F32),
            pltpu.VMEM((2, width, chan_a), F32),
            pltpu.VMEM((ar_total, 1, 2 * TILE), F32),
            pltpu.VMEM((ar_total, groups - 1, 1, 2 * TILE), F32),
            pltpu.VMEM((layers - 1, 2, EARLY_A * width, chan_a), F32),
            pltpu.VMEM((EARLY_A * width, chan_a), F32),
            pltpu.VMEM((2, EARLY_B * half_w, chan_m), F32),
            pltpu.SemaphoreType.DMA((5,)),
            pltpu.SemaphoreType.DMA((2, CHUNKS)),
            pltpu.SemaphoreType.DMA((2, CHUNKS)),
            pltpu.SemaphoreType.DMA((2, CHUNKS)),
            pltpu.SemaphoreType.DMA((2, CHUNKS)),
            pltpu.SemaphoreType.DMA((2, CHUNKS)),
            pltpu.SemaphoreType.DMA((ar_total,)),
            pltpu.SemaphoreType.DMA((ar_total,)),
            pltpu.SemaphoreType.DMA((layers + 1, 2)),
            pltpu.SemaphoreType.DMA((layers + 1, 2)),
            pltpu.SemaphoreType.DMA((3,)),
        ]
        return kernel, scratch, points

    def forward(images, w_a, bn_a, w_down, bn_down, w_in, bn_in, w_mid, bn_mid, w_out, bn_out):
        batch, rows, width, chan_a = images.shape
        chan_b, chan_m = w_in.shape[1:]
        kernel, scratch, points = make_kernel(batch, rows, width, chan_a, chan_b, chan_m, w_a.shape[0], w_in.shape[0])
        hbm = pl.BlockSpec(memory_space=pl.ANY)
        vmem = pl.BlockSpec(memory_space=pltpu.VMEM)
        h_last, branch, moments = pl.pallas_call(
            kernel,
            out_shape=(jax.ShapeDtypeStruct((points, chan_b), BF16),
                       jax.ShapeDtypeStruct((points, chan_m), BF16),
                       jax.ShapeDtypeStruct((8, chan_b), F32)),
            in_specs=[hbm] * 6 + [vmem] * 5,
            out_specs=(hbm, hbm, hbm),
            scratch_shapes=scratch,
            name="conv_stack",
            compiler_params=pltpu.CompilerParams(collective_id=0, has_side_effects=True, vmem_limit_bytes=67043328),
        )(images, w_a, w_down, w_in, w_mid, w_out, bn_a, bn_down, bn_in, bn_mid, bn_out)

        step = points // LAST_STEPS
        last = w_out.shape[0] - 1

        def finish(branch_ref, h_ref, w_ref, nrm_ref, out_ref):
            for t in range(chan_b // TILE):
                cols = slice(t * TILE, (t + 1) * TILE)
                z = jnp.dot(branch_ref[...], w_ref[0, :, cols], preferred_element_type=F32)
                normed = (z - nrm_ref[0:1, cols]) * nrm_ref[1:2, cols] + nrm_ref[2:3, cols]
                out_ref[:, cols] = jnp.maximum(normed + h_ref[:, cols].astype(F32), 0.0).astype(BF16)

        res = pl.pallas_call(
            finish,
            grid=(LAST_STEPS,),
            out_shape=jax.ShapeDtypeStruct((points, chan_b), BF16),
            in_specs=[pl.BlockSpec((step, chan_m), lambda i: (i, 0)),
                      pl.BlockSpec((step, chan_b), lambda i: (i, 0)),
                      pl.BlockSpec((1, chan_m, chan_b), lambda i: (last, 0, 0)),
                      pl.BlockSpec((8, chan_b), lambda i: (0, 0))],
            out_specs=pl.BlockSpec((step, chan_b), lambda i: (i, 0)),
            name="last_norm",
        )(branch, h_last, w_out, moments)
        return res.reshape(batch, rows // 2, width // 2, chan_b)

    act_spec = P("dp", "sp", None, None)
    return jax.shard_map(forward, mesh=mesh, in_specs=(act_spec,) + (P(),) * 10, out_specs=act_spec, check_vma=False)
```

```python
import jax
import jax.numpy as jnp
from jax import lax
from jax.experimental import pallas as pl
from jax.experimental.pallas import tpu as pltpu
from jax.sharding import PartitionSpec as P

NORM_EPS = 1e-5
CHUNKS = 16
ROW_STEPS = 8
IN_STEPS = 4
OUT_STEPS = 2
LAST_STEPS = 4
EARLY_A = 4
EARLY_B = 4
TILE = 256
F32 = jnp.float32
BF16 = jnp.bfloat16


def solution(mesh):
    groups = mesh.shape["sp"]
    peers = sorted(range(1, groups), key=lambda k: (abs(2 * k - groups), k))

    def make_kernel(batch, rows, width, chan_a, chan_b, chan_m, layers, blocks):
        half_w = width // 2
        points = batch * half_w
        per_chunk = batch // CHUNKS
        half_b = batch // 2
        tiles = chan_b // TILE
        m_rows = points // CHUNKS
        pair_a = 2 * chan_a
        early_a = EARLY_A // per_chunk
        early_b = EARLY_B // per_chunk
        count_a = float(batch * rows * width * groups)
        count_b = float(points * groups)
        messages = tuple((t,) for t in range(tiles))
        ar_in = layers
        ar_mid = ar_in + blocks
        ar_out = ar_mid + blocks
        ar_total = ar_out + (blocks + 1) * tiles

        def kernel(images, w_a, w_down, w_in, w_mid, w_out, bn_a, bn_down, bn_in, bn_mid, bn_out, h_out, u2_out, nrm_out,
                   xa, u, zb, h, u2, wa, wd, win, wmid, wout, st, nrm, prm, tmp, arsend, arbuf, ez_a, ez_d, ez_b,
                   sem_w, sem_img, a_send, a_recv, u_send, u_recv, ar_ssem, ar_rsem, e_send, e_recv, sem_out):
            me = lax.axis_index("sp")
            has_prev = me > 0
            has_next = me < groups - 1
            prev = jnp.maximum(me - 1, 0)
            nxt = jnp.minimum(me + 1, groups - 1)

            def remote(src, dst, ssem, rsem, dev):
                return pltpu.make_async_remote_copy(src_ref=src, dst_ref=dst, send_sem=ssem, recv_sem=rsem,
                                                    device_id={"sp": dev}, device_id_type=pl.DeviceIdType.MESH)

            barrier = pltpu.get_barrier_semaphore()
            for k in peers:
                pl.semaphore_signal(barrier, inc=1, device_id={"sp": lax.rem(me + k, groups)}, device_id_type=pl.DeviceIdType.MESH)

            def img_copy(c, r):
                sl = pl.ds(c * per_chunk, per_chunk)
                return pltpu.make_async_copy(images.at[sl, r], xa.at[1 + r, sl], sem_img.at[r, c])

            def load_images(c, _):
                for r in range(2):
                    img_copy(c, r).start()
                return 0
            lax.fori_loop(0, CHUNKS, load_images, 0)

            def wa_copies(start):
                for l in range(layers):
                    for dx in range(3):
                        for r in range(2):
                            for dy in range(3):
                                part = wa.at[l, pl.ds((r + dy) * chan_a, chan_a), pl.ds((2 * dx + r) * chan_a, chan_a)]
                                copy = pltpu.make_async_copy(w_a.at[l, dy, dx], part, sem_w.at[0])
                                if start:
                                    copy.start()
                                else:
                                    copy.wait()
            wa_copies(True)

            for l in range(layers):
                for dx in range(3):
                    for r in range(2):
                        wa[l, 3 * (1 - r) * chan_a:(3 * (1 - r) + 1) * chan_a, (2 * dx + r) * chan_a:(2 * dx + r + 1) * chan_a] = jnp.zeros((chan_a, chan_a), BF16)
            nrm[...] = jnp.zeros_like(nrm)
            prm[0] = bn_down[...]
            for j in range(blocks):
                prm[j + 1] = bn_out[j]

            pl.semaphore_wait(barrier, groups - 1)

            def a_copies(c, first):
                sl = pl.ds(c * per_chunk, per_chunk)
                top = images.at[sl, 0] if first else xa.at[1, sl]
                bot = images.at[sl, 1] if first else xa.at[2, sl]
                up = remote(top, xa.at[3, sl], a_send.at[0, c], a_recv.at[1, c], prev)
                down = remote(bot, xa.at[0, sl], a_send.at[1, c], a_recv.at[0, c], nxt)
                return up, down

            def d_copy(c):
                sl = pl.ds(c * per_chunk, per_chunk)
                return remote(u.at[0, sl], u.at[2, sl], u_send.at[0, c], u_recv.at[1, c], prev)

            def u_copies(c):
                sl = pl.ds(c * per_chunk, per_chunk)
                up = remote(u.at[1, sl], u.at[2, sl], u_send.at[0, c], u_recv.at[1, c], prev)
                down = remote(u.at[1, sl], u.at[0, sl], u_send.at[1, c], u_recv.at[0, c], nxt)
                return up, down

            def start_pair(up, down):
                @pl.when(has_prev)
                def _():
                    up.start()

                @pl.when(has_next)
                def _():
                    down.start()

            def wait_sends(pair_of, first=0):
                def body(c, _):
                    up, down = pair_of(c)

                    @pl.when(has_prev)
                    def _():
                        up.wait_send()

                    @pl.when(has_next)
                    def _():
                        down.wait_send()
                    return 0
                lax.fori_loop(first, CHUNKS, body, 0)

            def early_a_copies(l):
                rows_at = pl.ds(0, EARLY_A * width)
                if l == layers - 1:
                    return remote(zb.at[rows_at, pl.ds(0, chan_a)], ez_d, e_send.at[l, 0], e_recv.at[l, 1], prev), None
                up = remote(zb.at[rows_at, pl.ds(0, chan_a)], ez_a.at[l, 1], e_send.at[l, 0], e_recv.at[l, 1], prev)
                down = remote(zb.at[rows_at, pl.ds(chan_a, chan_a)], ez_a.at[l, 0], e_send.at[l, 1], e_recv.at[l, 0], nxt)
                return up, down

            def early_b_copies():
                src = zb.at[pl.ds(0, EARLY_B * half_w), pl.ds(0, chan_m)]
                up = remote(src, ez_b.at[1], e_send.at[layers, 0], e_recv.at[layers, 1], prev)
                down = remote(src, ez_b.at[0], e_send.at[layers, 1], e_recv.at[layers, 0], nxt)
                return up, down

            def start_early(up, down):
                @pl.when(has_prev)
                def _():
                    up.start()
                if down is not None:
                    @pl.when(has_next)
                    def _():
                        down.start()

            def sent_early(up, down):
                @pl.when(has_prev)
                def _():
                    up.wait_send()
                if down is not None:
                    @pl.when(has_next)
                    def _():
                        down.wait_send()

            def take_early(up, down, from_prev, from_next, count):
                if down is not None:
                    @pl.when(has_prev)
                    def _():
                        down.wait_recv()
                        lax.fori_loop(0, count, from_prev, 0)

                @pl.when(has_next)
                def _():
                    up.wait_recv()
                    lax.fori_loop(0, count, from_next, 0)

            def wait_halo(pair_of, c):
                up, down = pair_of(c)

                @pl.when(has_prev)
                def _():
                    down.wait_recv()

                @pl.when(has_next)
                def _():
                    up.wait_recv()

            def clear_moments():
                st[...] = jnp.zeros_like(st)

            def add_moments(z, lo):
                wide = z.shape[-1]
                part = min(512, z.shape[0])
                for p in range(0, z.shape[0], part):
                    z8 = z[p:p + part].reshape(part // 8, 8, wide)
                    st[0, :, lo:lo + wide] += jnp.sum(z8, axis=0)
                    st[1, :, lo:lo + wide] += jnp.sum(z8 * z8, axis=0)

            def ar_copy(a, k):
                return remote(arsend.at[a], arbuf.at[a, k - 1], ar_ssem.at[a], ar_rsem.at[a], lax.rem(me + k, groups))

            def pack_moments(a, lo):
                s = jnp.sum(st[0, :, lo:lo + TILE], axis=0, keepdims=True)
                q = jnp.sum(st[1, :, lo:lo + TILE], axis=0, keepdims=True)
                arsend[a] = jnp.concatenate([s, q], axis=1)

            def send_moments(a, lo):
                pack_moments(a, lo)
                for k in peers:
                    ar_copy(a, k).start()

            def ar_wait(a, sem):
                pltpu.make_async_copy(arbuf.at[a], arbuf.at[a], sem.at[a]).wait()

            def use_moments(a, params, lo, count):
                total = jnp.sum(arbuf[a], axis=0) + arsend[a]
                s = total[:, :TILE]
                q = total[:, TILE:]
                if count == count_a:
                    s = s[:, :chan_a] + s[:, chan_a:]
                    q = q[:, :chan_a] + q[:, chan_a:]
                m = s / count
                v = q / count - m * m
                scale = params[0:1] * lax.rsqrt(v + NORM_EPS)
                for at in range(lo, lo + TILE, m.shape[1]):
                    nrm[0:1, at:at + m.shape[1]] = m
                    nrm[1:2, at:at + m.shape[1]] = scale
                    nrm[2:3, at:at + m.shape[1]] = params[1:2]

            def recv_moments(a, params, lo, count):
                ar_wait(a, ar_rsem)
                use_moments(a, params, lo, count)
                ar_wait(a, ar_ssem)

            def send_tiles(first, ts):
                for t in ts:
                    pack_moments(first + t, t * TILE)
                at = pl.ds(first + ts[0], len(ts))
                for k in peers:
                    remote(arsend.at[at], arbuf.at[at, k - 1], ar_ssem.at[first + ts[0]], ar_rsem.at[first + ts[0]], lax.rem(me + k, groups)).start()

            def tile_waits(j, t, sem):
                first = ar_out + j * tiles

                if t == 0:
                    @pl.when(j == 0)
                    def _():
                        every = arbuf.at[pl.ds(ar_out, tiles)]
                        pltpu.make_async_copy(every, every, sem.at[ar_out]).wait()

                for ts in messages:
                    if t == ts[0]:
                        @pl.when(j > 0)
                        def _():
                            part = arbuf.at[pl.ds(first + t, len(ts))]
                            pltpu.make_async_copy(part, part, sem.at[first + t]).wait()

            def recv_tile(j, t):
                tile_waits(j, t, ar_rsem)
                use_moments(ar_out + j * tiles + t, prm[j, :, t * TILE:(t + 1) * TILE], t * TILE, count_b)
                tile_waits(j, t, ar_ssem)

            def norm(z, lo):
                wide = z.shape[-1]
                return (z - nrm[0:1, lo:lo + wide]) * nrm[1:2, lo:lo + wide] + nrm[2:3, lo:lo + wide]

            def norm_relu(z, lo):
                return jnp.maximum(norm(z, lo), 0.0)

            def from_left(y, wide):
                col = lax.broadcasted_iota(jnp.int32, y.shape, 0)
                return jnp.where(lax.rem(col, wide) == 0, 0.0, pltpu.roll(y, 1, 0))

            def from_right(y, wide):
                col = lax.broadcasted_iota(jnp.int32, y.shape, 0)
                return jnp.where(lax.rem(col, wide) == wide - 1, 0.0, pltpu.roll(y, y.shape[0] - 1, 0))

            def dot(x, w):
                return jnp.dot(x, w, preferred_element_type=F32)

            @pl.when(me == 0)
            def _():
                def body(b, _):
                    xa[0, b] = jnp.zeros((width, chan_a), BF16)
                    return 0
                lax.fori_loop(0, batch, body, 0)

            @pl.when(me == groups - 1)
            def _():
                def body(b, _):
                    xa[3, b] = jnp.zeros((width, chan_a), BF16)
                    u[2, b] = jnp.zeros((half_w, 2 * chan_a), BF16)
                    return 0
                lax.fori_loop(0, batch, body, 0)

            def send_a(c, _):
                start_pair(*a_copies(c, True))
                return 0
            lax.fori_loop(0, CHUNKS, send_a, 0)

            for dy in range(3):
                for dx in range(3):
                    row = (2 * dy + dx) * chan_a if dx < 2 else (6 + dy) * chan_a
                    pltpu.make_async_copy(w_down.at[dy, dx], wd.at[pl.ds(row, chan_a)], sem_w.at[1]).start()
                    for j in range(blocks):
                        pltpu.make_async_copy(w_mid.at[j, dy, dx], wmid.at[j, pl.ds(dy * chan_m, chan_m), pl.ds(dx * chan_m, chan_m)], sem_w.at[3]).start()
            pltpu.make_async_copy(w_in, win, sem_w.at[2]).start()
            pltpu.make_async_copy(w_out, wout, sem_w.at[4]).start()

            def wait_weight(ref, i):
                pltpu.make_async_copy(ref, ref, sem_w.at[i]).wait()

            wa_copies(False)

            def zero_h(c, _):
                h[pl.ds(pl.multiple_of(c * m_rows, m_rows), m_rows), :] = jnp.zeros((m_rows, chan_b), BF16)
                return 0
            lax.fori_loop(0, CHUNKS, zero_h, 0)

            def conv_a(l):
                clear_moments()
                for hb in range(2):
                    def body(i, _):
                        b = hb * half_b + i
                        c = b // per_chunk

                        @pl.when(jnp.logical_and(lax.rem(b, per_chunk) == 0, c >= (early_a if l else 0)))
                        def _():
                            if l == 0:
                                for r in range(2):
                                    img_copy(c, r).wait()
                            wait_halo(lambda c: a_copies(c, l == 0), c)
                        x = jnp.concatenate([xa[r, b] for r in range(4)], axis=1)
                        z = dot(x, wa[l, :, pair_a:2 * pair_a])
                        z = z + from_left(dot(x, wa[l, :, 0:pair_a]), width)
                        z = z + from_right(dot(x, wa[l, :, 2 * pair_a:3 * pair_a]), width)
                        zb[pl.ds(pl.multiple_of(i * width, width), width), hb * pair_a:(hb + 1) * pair_a] = z
                        add_moments(z, 0)
                        return 0
                    lax.fori_loop(0, half_b, body, 0)
                send_moments(l, 0)
                start_early(*early_a_copies(l))
                wait_sends(lambda c: a_copies(c, l == 0), early_a if l else 0)
                recv_moments(l, bn_a[l], 0, count_a)

            def normed_pair(hb, i):
                z = zb[pl.ds(pl.multiple_of(i * width, width), width), hb * pair_a:(hb + 1) * pair_a]
                return norm_relu(z, 0)

            conv_a(0)
            for l in range(1, layers):
                for hb in range(2):
                    def renorm(i, _):
                        b = hb * half_b + i
                        y = normed_pair(hb, i).astype(BF16)
                        xa[1, b] = y[:, :chan_a]
                        xa[2, b] = y[:, chan_a:]

                        @pl.when(jnp.logical_and(lax.rem(b, per_chunk) == per_chunk - 1, b >= EARLY_A))
                        def _():
                            start_pair(*a_copies(b // per_chunk, False))
                        return 0
                    lax.fori_loop(0, half_b, renorm, 0)

                def early_rows(side, slot):
                    def body(b, _):
                        z = ez_a[l - 1, side, pl.ds(pl.multiple_of(b * width, width), width), :]
                        xa[slot, b] = norm_relu(z, 0).astype(BF16)
                        return 0
                    return body
                up, down = early_a_copies(l - 1)
                take_early(up, down, early_rows(0, 0), early_rows(1, 3), EARLY_A)
                sent_early(up, down)
                conv_a(l)

            for hb in range(2):
                def pair_up(i, _):
                    b = hb * half_b + i
                    y = normed_pair(hb, i)
                    for r in range(2):
                        tmp[r] = y[:, r * chan_a:(r + 1) * chan_a]
                        u[r, b, :, 0:chan_a] = tmp[r, pl.ds(0, half_w, stride=2), :].astype(BF16)
                        u[r, b, :, chan_a:2 * chan_a] = tmp[r, pl.ds(1, half_w, stride=2), :].astype(BF16)

                    @pl.when(jnp.logical_and(jnp.logical_and(lax.rem(b, per_chunk) == per_chunk - 1, b >= EARLY_A), has_prev))
                    def _():
                        d_copy(b // per_chunk).start()
                    return 0
                lax.fori_loop(0, half_b, pair_up, 0)

            def early_pair(b, _):
                tmp[0] = norm_relu(ez_d[pl.ds(pl.multiple_of(b * width, width), width), :], 0)
                u[2, b, :, 0:chan_a] = tmp[0, pl.ds(0, half_w, stride=2), :].astype(BF16)
                u[2, b, :, chan_a:2 * chan_a] = tmp[0, pl.ds(1, half_w, stride=2), :].astype(BF16)
                return 0
            up, down = early_a_copies(layers - 1)
            take_early(up, down, None, early_pair, EARLY_A)
            sent_early(up, down)
            wait_weight(wd, 1)
            clear_moments()

            def down_body(c, _):
                @pl.when(jnp.logical_and(has_next, c >= early_a))
                def _():
                    d_copy(c).wait_recv()
                sl = pl.ds(c * per_chunk, per_chunk)
                flat = [u[r, sl].reshape(m_rows, 2 * chan_a) for r in range(3)]
                evens = [from_right(f[:, :chan_a].astype(F32), half_w).astype(BF16) for f in flat]
                x = jnp.concatenate(flat + evens, axis=1)
                rows_at = pl.ds(pl.multiple_of(c * m_rows, m_rows), m_rows)
                for t in range(tiles):
                    z = dot(x, wd[:, t * TILE:(t + 1) * TILE])
                    zb[rows_at, t * TILE:(t + 1) * TILE] = z
                    add_moments(z, t * TILE)
                return 0
            lax.fori_loop(0, CHUNKS, down_body, 0)
            send_tiles(ar_out, tuple(range(tiles)))

            def wait_d(c, _):
                @pl.when(has_prev)
                def _():
                    d_copy(c).wait_send()
                return 0
            lax.fori_loop(early_a, CHUNKS, wait_d, 0)

            @pl.when(me == 0)
            def _():
                def body(b, _):
                    u[0, b] = jnp.zeros((half_w, chan_m), BF16)
                    return 0
                lax.fori_loop(0, batch, body, 0)

            wait_weight(win, 2)
            wait_weight(wmid, 3)
            wait_weight(wout, 4)

            def next_h(rows_at, t):
                cols = slice(t * TILE, (t + 1) * TILE)
                summed = norm(zb[rows_at, cols], t * TILE) + h[rows_at, cols].astype(F32)
                return jnp.maximum(summed, 0.0).astype(BF16)

            def h_copy():
                return pltpu.make_async_copy(h, h_out, sem_out.at[0])

            def u2_copy():
                return pltpu.make_async_copy(u2, u2_out, sem_out.at[1])

            def block(j, _):
                for t in range(tiles - 1):
                    recv_tile(j, t)

                    def tile_body(c, _):
                        rows_at = pl.ds(pl.multiple_of(c * (points // ROW_STEPS), points // ROW_STEPS), points // ROW_STEPS)
                        h[rows_at, t * TILE:(t + 1) * TILE] = next_h(rows_at, t)
                        return 0
                    lax.fori_loop(0, ROW_STEPS, tile_body, 0)
                recv_tile(j, tiles - 1)
                clear_moments()

                def in_body(c, _):
                    rows_at = pl.ds(pl.multiple_of(c * (points // IN_STEPS), points // IN_STEPS), points // IN_STEPS)
                    last = next_h(rows_at, tiles - 1)
                    h[rows_at, chan_b - TILE:chan_b] = last
                    z = dot(jnp.concatenate([h[rows_at, 0:chan_b - TILE], last], axis=1), win[j])
                    zb[rows_at, 0:chan_m] = z
                    add_moments(z, 0)
                    return 0
                lax.fori_loop(0, IN_STEPS, in_body, 0)
                send_moments(ar_in + j, 0)
                start_early(*early_b_copies())

                @pl.when(j == blocks - 1)
                def _():
                    h_copy().start()
                recv_moments(ar_in + j, bn_in[j], 0, count_b)

                def renorm_u(c, _):
                    rows_at = pl.ds(pl.multiple_of(c * m_rows, m_rows), m_rows)
                    sl = pl.ds(c * per_chunk, per_chunk)
                    u[1, sl] = norm_relu(zb[rows_at, 0:chan_m], 0).astype(BF16).reshape(per_chunk, half_w, chan_m)

                    @pl.when(c >= early_b)
                    def _():
                        start_pair(*u_copies(c))
                    return 0
                lax.fori_loop(0, CHUNKS, renorm_u, 0)

                def early_u(side, slot):
                    def body(b, _):
                        z = ez_b[side, pl.ds(pl.multiple_of(b * half_w, half_w), half_w), :]
                        u[slot, b] = norm_relu(z, 0).astype(BF16)
                        return 0
                    return body
                up, down = early_b_copies()
                take_early(up, down, early_u(0, 0), early_u(1, 2), EARLY_B)
                sent_early(up, down)
                clear_moments()

                def mid_body(c, _):
                    @pl.when(c >= early_b)
                    def _():
                        wait_halo(u_copies, c)
                    rows_at = pl.ds(pl.multiple_of(c * m_rows, m_rows), m_rows)
                    sl = pl.ds(c * per_chunk, per_chunk)
                    x = jnp.concatenate([u[r, sl].reshape(m_rows, chan_m) for r in range(3)], axis=1)
                    z = dot(x, wmid[j, :, chan_m:2 * chan_m])
                    z = z + from_left(dot(x, wmid[j, :, 0:chan_m]), half_w)
                    z = z + from_right(dot(x, wmid[j, :, 2 * chan_m:3 * chan_m]), half_w)
                    zb[rows_at, 0:chan_m] = z
                    add_moments(z, 0)
                    return 0
                lax.fori_loop(0, CHUNKS, mid_body, 0)
                send_moments(ar_mid + j, 0)
                wait_sends(u_copies, early_b)
                recv_moments(ar_mid + j, bn_mid[j], 0, count_b)

                clear_moments()
                for t in range(tiles):
                    cols = slice(t * TILE, (t + 1) * TILE)

                    def out_body(c, _):
                        rows_at = pl.ds(c * (points // OUT_STEPS), points // OUT_STEPS)
                        if t == 0:
                            u2[rows_at, :] = norm_relu(zb[rows_at, 0:chan_m], 0).astype(BF16)
                        z = dot(u2[rows_at, :], wout[j, :, cols])
                        zb[rows_at, cols] = z
                        add_moments(z, t * TILE)
                        return 0
                    for c in range(OUT_STEPS):
                        out_body(c, 0)
                    for ts in messages:
                        if t == ts[-1]:
                            send_tiles(ar_out + (j + 1) * tiles, ts)
                    if t == 0:
                        @pl.when(j == blocks - 1)
                        def _():
                            u2_copy().start()
                return 0
            lax.fori_loop(0, blocks, block, 0)

            for t in range(tiles):
                recv_tile(blocks, t)
            nrm_copy = pltpu.make_async_copy(nrm, nrm_out, sem_out.at[2])
            nrm_copy.start()
            h_copy().wait()
            u2_copy().wait()
            nrm_copy.wait()

        scratch = [
            pltpu.VMEM((4, batch, width, chan_a), BF16),
            pltpu.VMEM((3, batch, half_w, chan_m), BF16),
            pltpu.VMEM((points, chan_b), F32),
            pltpu.VMEM((points, chan_b), BF16),
            pltpu.VMEM((points, chan_m), BF16),
            pltpu.VMEM((layers, 4 * chan_a, 6 * chan_a), BF16),
            pltpu.VMEM((9 * chan_a, chan_b), BF16),
            pltpu.VMEM((blocks, chan_b, chan_m), BF16),
            pltpu.VMEM((blocks, 3 * chan_m, 3 * chan_m), BF16),
            pltpu.VMEM((blocks, chan_m, chan_b), BF16),
            pltpu.VMEM((2, 8, chan_b), F32),
            pltpu.VMEM((8, chan_b), F32),
            pltpu.VMEM((blocks + 1, 2, chan_b), F32),
            pltpu.VMEM((2, width, chan_a), F32),
            pltpu.VMEM((ar_total, 1, 2 * TILE), F32),
            pltpu.VMEM((ar_total, groups - 1, 1, 2 * TILE), F32),
            pltpu.VMEM((layers - 1, 2, EARLY_A * width, chan_a), F32),
            pltpu.VMEM((EARLY_A * width, chan_a), F32),
            pltpu.VMEM((2, EARLY_B * half_w, chan_m), F32),
            pltpu.SemaphoreType.DMA((5,)),
            pltpu.SemaphoreType.DMA((2, CHUNKS)),
            pltpu.SemaphoreType.DMA((2, CHUNKS)),
            pltpu.SemaphoreType.DMA((2, CHUNKS)),
            pltpu.SemaphoreType.DMA((2, CHUNKS)),
            pltpu.SemaphoreType.DMA((2, CHUNKS)),
            pltpu.SemaphoreType.DMA((ar_total,)),
            pltpu.SemaphoreType.DMA((ar_total,)),
            pltpu.SemaphoreType.DMA((layers + 1, 2)),
            pltpu.SemaphoreType.DMA((layers + 1, 2)),
            pltpu.SemaphoreType.DMA((3,)),
        ]
        return kernel, scratch, points

    def forward(images, w_a, bn_a, w_down, bn_down, w_in, bn_in, w_mid, bn_mid, w_out, bn_out):
        batch, rows, width, chan_a = images.shape
        chan_b, chan_m = w_in.shape[1:]
        kernel, scratch, points = make_kernel(batch, rows, width, chan_a, chan_b, chan_m, w_a.shape[0], w_in.shape[0])
        hbm = pl.BlockSpec(memory_space=pl.ANY)
        vmem = pl.BlockSpec(memory_space=pltpu.VMEM)
        h_last, branch, moments = pl.pallas_call(
            kernel,
            out_shape=(jax.ShapeDtypeStruct((points, chan_b), BF16),
                       jax.ShapeDtypeStruct((points, chan_m), BF16),
                       jax.ShapeDtypeStruct((8, chan_b), F32)),
            in_specs=[hbm] * 6 + [vmem] * 5,
            out_specs=(hbm, hbm, hbm),
            scratch_shapes=scratch,
            name="conv_stack",
            compiler_params=pltpu.CompilerParams(collective_id=0, has_side_effects=True, vmem_limit_bytes=67043328),
        )(images, w_a, w_down, w_in, w_mid, w_out, bn_a, bn_down, bn_in, bn_mid, bn_out)

        step = points // LAST_STEPS
        last = w_out.shape[0] - 1

        def finish(branch_ref, h_ref, w_ref, nrm_ref, out_ref):
            for t in range(chan_b // TILE):
                cols = slice(t * TILE, (t + 1) * TILE)
                z = jnp.dot(branch_ref[...], w_ref[0, :, cols], preferred_element_type=F32)
                normed = (z - nrm_ref[0:1, cols]) * nrm_ref[1:2, cols] + nrm_ref[2:3, cols]
                out_ref[:, cols] = jnp.maximum(normed + h_ref[:, cols].astype(F32), 0.0).astype(BF16)

        res = pl.pallas_call(
            finish,
            grid=(LAST_STEPS,),
            out_shape=jax.ShapeDtypeStruct((points, chan_b), BF16),
            in_specs=[pl.BlockSpec((step, chan_m), lambda i: (i, 0)),
                      pl.BlockSpec((step, chan_b), lambda i: (i, 0)),
                      pl.BlockSpec((1, chan_m, chan_b), lambda i: (last, 0, 0)),
                      pl.BlockSpec((8, chan_b), lambda i: (0, 0))],
            out_specs=pl.BlockSpec((step, chan_b), lambda i: (i, 0)),
            name="last_norm",
        )(branch, h_last, w_out, moments)
        return res.reshape(batch, rows // 2, width // 2, chan_b)

    act_spec = P("dp", "sp", None, None)
    return jax.shard_map(forward, mesh=mesh, in_specs=(act_spec,) + (P(),) * 10, out_specs=act_spec, check_vma=False)
```

```python
import jax
import jax.numpy as jnp
from jax import lax
from jax.experimental import pallas as pl
from jax.experimental.pallas import tpu as pltpu
from jax.sharding import PartitionSpec as P

NORM_EPS = 1e-5
CHUNKS = 16
ROW_STEPS = 8
IN_STEPS = 4
OUT_STEPS = 2
LAST_STEPS = 2
EARLY_A = 4
EARLY_B = 4
TILE = 256
F32 = jnp.float32
BF16 = jnp.bfloat16


def solution(mesh):
    groups = mesh.shape["sp"]
    peers = sorted(range(1, groups), key=lambda k: (abs(2 * k - groups), k))

    def make_kernel(batch, rows, width, chan_a, chan_b, chan_m, layers, blocks):
        half_w = width // 2
        points = batch * half_w
        per_chunk = batch // CHUNKS
        half_b = batch // 2
        tiles = chan_b // TILE
        m_rows = points // CHUNKS
        pair_a = 2 * chan_a
        early_a = EARLY_A // per_chunk
        early_b = EARLY_B // per_chunk
        count_a = float(batch * rows * width * groups)
        count_b = float(points * groups)
        messages = tuple((t,) for t in range(tiles))
        ar_in = layers
        ar_mid = ar_in + blocks
        ar_out = ar_mid + blocks
        ar_total = ar_out + (blocks + 1) * tiles

        def kernel(images, w_a, w_down, w_in, w_mid, w_out, bn_a, bn_down, bn_in, bn_mid, bn_out, h_out, u2_out, nrm_out,
                   xa, u, zb, h, u2, wa, wd, win, wmid, wout, st, nrm, prm, tmp, arsend, arbuf, ez_a, ez_d, ez_b,
                   sem_w, sem_img, a_send, a_recv, u_send, u_recv, ar_ssem, ar_rsem, e_send, e_recv, sem_out):
            me = lax.axis_index("sp")
            has_prev = me > 0
            has_next = me < groups - 1
            prev = jnp.maximum(me - 1, 0)
            nxt = jnp.minimum(me + 1, groups - 1)

            def remote(src, dst, ssem, rsem, dev):
                return pltpu.make_async_remote_copy(src_ref=src, dst_ref=dst, send_sem=ssem, recv_sem=rsem,
                                                    device_id={"sp": dev}, device_id_type=pl.DeviceIdType.MESH)

            barrier = pltpu.get_barrier_semaphore()
            for k in peers:
                pl.semaphore_signal(barrier, inc=1, device_id={"sp": lax.rem(me + k, groups)}, device_id_type=pl.DeviceIdType.MESH)

            def img_copy(c, r):
                sl = pl.ds(c * per_chunk, per_chunk)
                return pltpu.make_async_copy(images.at[sl, r], xa.at[1 + r, sl], sem_img.at[r, c])

            def load_images(c, _):
                for r in range(2):
                    img_copy(c, r).start()
                return 0
            lax.fori_loop(0, CHUNKS, load_images, 0)

            def wa_copies(start):
                for l in range(layers):
                    for dx in range(3):
                        for r in range(2):
                            for dy in range(3):
                                part = wa.at[l, pl.ds((r + dy) * chan_a, chan_a), pl.ds((2 * dx + r) * chan_a, chan_a)]
                                copy = pltpu.make_async_copy(w_a.at[l, dy, dx], part, sem_w.at[0])
                                if start:
                                    copy.start()
                                else:
                                    copy.wait()
            wa_copies(True)

            for l in range(layers):
                for dx in range(3):
                    for r in range(2):
                        wa[l, 3 * (1 - r) * chan_a:(3 * (1 - r) + 1) * chan_a, (2 * dx + r) * chan_a:(2 * dx + r + 1) * chan_a] = jnp.zeros((chan_a, chan_a), BF16)
            nrm[...] = jnp.zeros_like(nrm)
            prm[0] = bn_down[...]
            for j in range(blocks):
                prm[j + 1] = bn_out[j]

            pl.semaphore_wait(barrier, groups - 1)

            def a_copies(c, first):
                sl = pl.ds(c * per_chunk, per_chunk)
                top = images.at[sl, 0] if first else xa.at[1, sl]
                bot = images.at[sl, 1] if first else xa.at[2, sl]
                up = remote(top, xa.at[3, sl], a_send.at[0, c], a_recv.at[1, c], prev)
                down = remote(bot, xa.at[0, sl], a_send.at[1, c], a_recv.at[0, c], nxt)
                return up, down

            def d_copy(c):
                sl = pl.ds(c * per_chunk, per_chunk)
                return remote(u.at[0, sl], u.at[2, sl], u_send.at[0, c], u_recv.at[1, c], prev)

            def u_copies(c):
                sl = pl.ds(c * per_chunk, per_chunk)
                up = remote(u.at[1, sl], u.at[2, sl], u_send.at[0, c], u_recv.at[1, c], prev)
                down = remote(u.at[1, sl], u.at[0, sl], u_send.at[1, c], u_recv.at[0, c], nxt)
                return up, down

            def start_pair(up, down):
                @pl.when(has_prev)
                def _():
                    up.start()

                @pl.when(has_next)
                def _():
                    down.start()

            def wait_sends(pair_of, first=0):
                def body(c, _):
                    up, down = pair_of(c)

                    @pl.when(has_prev)
                    def _():
                        up.wait_send()

                    @pl.when(has_next)
                    def _():
                        down.wait_send()
                    return 0
                lax.fori_loop(first, CHUNKS, body, 0)

            def early_a_copies(l):
                rows_at = pl.ds(0, EARLY_A * width)
                if l == layers - 1:
                    return remote(zb.at[rows_at, pl.ds(0, chan_a)], ez_d, e_send.at[l, 0], e_recv.at[l, 1], prev), None
                up = remote(zb.at[rows_at, pl.ds(0, chan_a)], ez_a.at[l, 1], e_send.at[l, 0], e_recv.at[l, 1], prev)
                down = remote(zb.at[rows_at, pl.ds(chan_a, chan_a)], ez_a.at[l, 0], e_send.at[l, 1], e_recv.at[l, 0], nxt)
                return up, down

            def early_b_copies():
                src = zb.at[pl.ds(0, EARLY_B * half_w), pl.ds(0, chan_m)]
                up = remote(src, ez_b.at[1], e_send.at[layers, 0], e_recv.at[layers, 1], prev)
                down = remote(src, ez_b.at[0], e_send.at[layers, 1], e_recv.at[layers, 0], nxt)
                return up, down

            def start_early(up, down):
                @pl.when(has_prev)
                def _():
                    up.start()
                if down is not None:
                    @pl.when(has_next)
                    def _():
                        down.start()

            def sent_early(up, down):
                @pl.when(has_prev)
                def _():
                    up.wait_send()
                if down is not None:
                    @pl.when(has_next)
                    def _():
                        down.wait_send()

            def take_early(up, down, from_prev, from_next, count):
                if down is not None:
                    @pl.when(has_prev)
                    def _():
                        down.wait_recv()
                        lax.fori_loop(0, count, from_prev, 0)

                @pl.when(has_next)
                def _():
                    up.wait_recv()
                    lax.fori_loop(0, count, from_next, 0)

            def wait_halo(pair_of, c):
                up, down = pair_of(c)

                @pl.when(has_prev)
                def _():
                    down.wait_recv()

                @pl.when(has_next)
                def _():
                    up.wait_recv()

            def clear_moments():
                st[...] = jnp.zeros_like(st)

            def add_moments(z, lo):
                wide = z.shape[-1]
                part = min(512, z.shape[0])
                for p in range(0, z.shape[0], part):
                    z8 = z[p:p + part].reshape(part // 8, 8, wide)
                    st[0, :, lo:lo + wide] += jnp.sum(z8, axis=0)
                    st[1, :, lo:lo + wide] += jnp.sum(z8 * z8, axis=0)

            def ar_copy(a, k):
                return remote(arsend.at[a], arbuf.at[a, k - 1], ar_ssem.at[a], ar_rsem.at[a], lax.rem(me + k, groups))

            def pack_moments(a, lo):
                s = jnp.sum(st[0, :, lo:lo + TILE], axis=0, keepdims=True)
                q = jnp.sum(st[1, :, lo:lo + TILE], axis=0, keepdims=True)
                arsend[a] = jnp.concatenate([s, q], axis=1)

            def send_moments(a, lo):
                pack_moments(a, lo)
                for k in peers:
                    ar_copy(a, k).start()

            def ar_wait(a, sem):
                pltpu.make_async_copy(arbuf.at[a], arbuf.at[a], sem.at[a]).wait()

            def use_moments(a, params, lo, count):
                total = jnp.sum(arbuf[a], axis=0) + arsend[a]
                s = total[:, :TILE]
                q = total[:, TILE:]
                if count == count_a:
                    s = s[:, :chan_a] + s[:, chan_a:]
                    q = q[:, :chan_a] + q[:, chan_a:]
                m = s / count
                v = q / count - m * m
                scale = params[0:1] * lax.rsqrt(v + NORM_EPS)
                for at in range(lo, lo + TILE, m.shape[1]):
                    nrm[0:1, at:at + m.shape[1]] = m
                    nrm[1:2, at:at + m.shape[1]] = scale
                    nrm[2:3, at:at + m.shape[1]] = params[1:2]

            def recv_moments(a, params, lo, count):
                ar_wait(a, ar_rsem)
                use_moments(a, params, lo, count)
                ar_wait(a, ar_ssem)

            def send_tiles(first, ts):
                for t in ts:
                    pack_moments(first + t, t * TILE)
                at = pl.ds(first + ts[0], len(ts))
                for k in peers:
                    remote(arsend.at[at], arbuf.at[at, k - 1], ar_ssem.at[first + ts[0]], ar_rsem.at[first + ts[0]], lax.rem(me + k, groups)).start()

            def tile_waits(j, t, sem):
                first = ar_out + j * tiles

                if t == 0:
                    @pl.when(j == 0)
                    def _():
                        every = arbuf.at[pl.ds(ar_out, tiles)]
                        pltpu.make_async_copy(every, every, sem.at[ar_out]).wait()

                for ts in messages:
                    if t == ts[0]:
                        @pl.when(j > 0)
                        def _():
                            part = arbuf.at[pl.ds(first + t, len(ts))]
                            pltpu.make_async_copy(part, part, sem.at[first + t]).wait()

            def recv_tile(j, t):
                tile_waits(j, t, ar_rsem)
                use_moments(ar_out + j * tiles + t, prm[j, :, t * TILE:(t + 1) * TILE], t * TILE, count_b)
                tile_waits(j, t, ar_ssem)

            def norm(z, lo):
                wide = z.shape[-1]
                return (z - nrm[0:1, lo:lo + wide]) * nrm[1:2, lo:lo + wide] + nrm[2:3, lo:lo + wide]

            def norm_relu(z, lo):
                return jnp.maximum(norm(z, lo), 0.0)

            def from_left(y, wide):
                col = lax.broadcasted_iota(jnp.int32, y.shape, 0)
                return jnp.where(lax.rem(col, wide) == 0, 0.0, pltpu.roll(y, 1, 0))

            def from_right(y, wide):
                col = lax.broadcasted_iota(jnp.int32, y.shape, 0)
                return jnp.where(lax.rem(col, wide) == wide - 1, 0.0, pltpu.roll(y, y.shape[0] - 1, 0))

            def dot(x, w):
                return jnp.dot(x, w, preferred_element_type=F32)

            @pl.when(me == 0)
            def _():
                def body(b, _):
                    xa[0, b] = jnp.zeros((width, chan_a), BF16)
                    return 0
                lax.fori_loop(0, batch, body, 0)

            @pl.when(me == groups - 1)
            def _():
                def body(b, _):
                    xa[3, b] = jnp.zeros((width, chan_a), BF16)
                    u[2, b] = jnp.zeros((half_w, 2 * chan_a), BF16)
                    return 0
                lax.fori_loop(0, batch, body, 0)

            def send_a(c, _):
                start_pair(*a_copies(c, True))
                return 0
            lax.fori_loop(0, CHUNKS, send_a, 0)

            for dy in range(3):
                for dx in range(3):
                    row = (2 * dy + dx) * chan_a if dx < 2 else (6 + dy) * chan_a
                    pltpu.make_async_copy(w_down.at[dy, dx], wd.at[pl.ds(row, chan_a)], sem_w.at[1]).start()
                    for j in range(blocks):
                        pltpu.make_async_copy(w_mid.at[j, dy, dx], wmid.at[j, pl.ds(dy * chan_m, chan_m), pl.ds(dx * chan_m, chan_m)], sem_w.at[3]).start()
            pltpu.make_async_copy(w_in, win, sem_w.at[2]).start()
            pltpu.make_async_copy(w_out, wout, sem_w.at[4]).start()

            def wait_weight(ref, i):
                pltpu.make_async_copy(ref, ref, sem_w.at[i]).wait()

            wa_copies(False)

            def zero_h(c, _):
                h[pl.ds(pl.multiple_of(c * m_rows, m_rows), m_rows), :] = jnp.zeros((m_rows, chan_b), BF16)
                return 0
            lax.fori_loop(0, CHUNKS, zero_h, 0)

            def conv_a(l):
                clear_moments()
                for hb in range(2):
                    def body(i, _):
                        b = hb * half_b + i
                        c = b // per_chunk

                        @pl.when(jnp.logical_and(lax.rem(b, per_chunk) == 0, c >= (early_a if l else 0)))
                        def _():
                            if l == 0:
                                for r in range(2):
                                    img_copy(c, r).wait()
                            wait_halo(lambda c: a_copies(c, l == 0), c)
                        x = jnp.concatenate([xa[r, b] for r in range(4)], axis=1)
                        z = dot(x, wa[l, :, pair_a:2 * pair_a])
                        z = z + from_left(dot(x, wa[l, :, 0:pair_a]), width)
                        z = z + from_right(dot(x, wa[l, :, 2 * pair_a:3 * pair_a]), width)
                        zb[pl.ds(pl.multiple_of(i * width, width), width), hb * pair_a:(hb + 1) * pair_a] = z
                        add_moments(z, 0)
                        return 0
                    lax.fori_loop(0, half_b, body, 0)
                send_moments(l, 0)
                start_early(*early_a_copies(l))
                wait_sends(lambda c: a_copies(c, l == 0), early_a if l else 0)
                recv_moments(l, bn_a[l], 0, count_a)

            def normed_pair(hb, i):
                z = zb[pl.ds(pl.multiple_of(i * width, width), width), hb * pair_a:(hb + 1) * pair_a]
                return norm_relu(z, 0)

            conv_a(0)
            for l in range(1, layers):
                for hb in range(2):
                    def renorm(i, _):
                        b = hb * half_b + i
                        y = normed_pair(hb, i).astype(BF16)
                        xa[1, b] = y[:, :chan_a]
                        xa[2, b] = y[:, chan_a:]

                        @pl.when(jnp.logical_and(lax.rem(b, per_chunk) == per_chunk - 1, b >= EARLY_A))
                        def _():
                            start_pair(*a_copies(b // per_chunk, False))
                        return 0
                    lax.fori_loop(0, half_b, renorm, 0)

                def early_rows(side, slot):
                    def body(b, _):
                        z = ez_a[l - 1, side, pl.ds(pl.multiple_of(b * width, width), width), :]
                        xa[slot, b] = norm_relu(z, 0).astype(BF16)
                        return 0
                    return body
                up, down = early_a_copies(l - 1)
                take_early(up, down, early_rows(0, 0), early_rows(1, 3), EARLY_A)
                sent_early(up, down)
                conv_a(l)

            for hb in range(2):
                def pair_up(i, _):
                    b = hb * half_b + i
                    y = normed_pair(hb, i)
                    for r in range(2):
                        tmp[r] = y[:, r * chan_a:(r + 1) * chan_a]
                        u[r, b, :, 0:chan_a] = tmp[r, pl.ds(0, half_w, stride=2), :].astype(BF16)
                        u[r, b, :, chan_a:2 * chan_a] = tmp[r, pl.ds(1, half_w, stride=2), :].astype(BF16)

                    @pl.when(jnp.logical_and(jnp.logical_and(lax.rem(b, per_chunk) == per_chunk - 1, b >= EARLY_A), has_prev))
                    def _():
                        d_copy(b // per_chunk).start()
                    return 0
                lax.fori_loop(0, half_b, pair_up, 0)

            def early_pair(b, _):
                tmp[0] = norm_relu(ez_d[pl.ds(pl.multiple_of(b * width, width), width), :], 0)
                u[2, b, :, 0:chan_a] = tmp[0, pl.ds(0, half_w, stride=2), :].astype(BF16)
                u[2, b, :, chan_a:2 * chan_a] = tmp[0, pl.ds(1, half_w, stride=2), :].astype(BF16)
                return 0
            up, down = early_a_copies(layers - 1)
            take_early(up, down, None, early_pair, EARLY_A)
            sent_early(up, down)
            wait_weight(wd, 1)
            clear_moments()

            def down_body(c, _):
                @pl.when(jnp.logical_and(has_next, c >= early_a))
                def _():
                    d_copy(c).wait_recv()
                sl = pl.ds(c * per_chunk, per_chunk)
                flat = [u[r, sl].reshape(m_rows, 2 * chan_a) for r in range(3)]
                evens = [from_right(f[:, :chan_a].astype(F32), half_w).astype(BF16) for f in flat]
                x = jnp.concatenate(flat + evens, axis=1)
                rows_at = pl.ds(pl.multiple_of(c * m_rows, m_rows), m_rows)
                for t in range(tiles):
                    z = dot(x, wd[:, t * TILE:(t + 1) * TILE])
                    zb[rows_at, t * TILE:(t + 1) * TILE] = z
                    add_moments(z, t * TILE)
                return 0
            lax.fori_loop(0, CHUNKS, down_body, 0)
            send_tiles(ar_out, tuple(range(tiles)))

            def wait_d(c, _):
                @pl.when(has_prev)
                def _():
                    d_copy(c).wait_send()
                return 0
            lax.fori_loop(early_a, CHUNKS, wait_d, 0)

            @pl.when(me == 0)
            def _():
                def body(b, _):
                    u[0, b] = jnp.zeros((half_w, chan_m), BF16)
                    return 0
                lax.fori_loop(0, batch, body, 0)

            wait_weight(win, 2)
            wait_weight(wmid, 3)
            wait_weight(wout, 4)

            def next_h(rows_at, t):
                cols = slice(t * TILE, (t + 1) * TILE)
                summed = norm(zb[rows_at, cols], t * TILE) + h[rows_at, cols].astype(F32)
                return jnp.maximum(summed, 0.0).astype(BF16)

            def h_copy():
                return pltpu.make_async_copy(h, h_out, sem_out.at[0])

            def u2_copy():
                return pltpu.make_async_copy(u2, u2_out, sem_out.at[1])

            def block(j, _):
                for t in range(tiles - 1):
                    recv_tile(j, t)

                    def tile_body(c, _):
                        rows_at = pl.ds(pl.multiple_of(c * (points // ROW_STEPS), points // ROW_STEPS), points // ROW_STEPS)
                        h[rows_at, t * TILE:(t + 1) * TILE] = next_h(rows_at, t)
                        return 0
                    lax.fori_loop(0, ROW_STEPS, tile_body, 0)
                recv_tile(j, tiles - 1)
                clear_moments()

                def in_body(c, _):
                    rows_at = pl.ds(pl.multiple_of(c * (points // IN_STEPS), points // IN_STEPS), points // IN_STEPS)
                    last = next_h(rows_at, tiles - 1)
                    h[rows_at, chan_b - TILE:chan_b] = last
                    z = dot(jnp.concatenate([h[rows_at, 0:chan_b - TILE], last], axis=1), win[j])
                    zb[rows_at, 0:chan_m] = z
                    add_moments(z, 0)
                    return 0
                lax.fori_loop(0, IN_STEPS, in_body, 0)
                send_moments(ar_in + j, 0)
                start_early(*early_b_copies())

                @pl.when(j == blocks - 1)
                def _():
                    h_copy().start()
                recv_moments(ar_in + j, bn_in[j], 0, count_b)

                def renorm_u(c, _):
                    rows_at = pl.ds(pl.multiple_of(c * m_rows, m_rows), m_rows)
                    sl = pl.ds(c * per_chunk, per_chunk)
                    u[1, sl] = norm_relu(zb[rows_at, 0:chan_m], 0).astype(BF16).reshape(per_chunk, half_w, chan_m)

                    @pl.when(c >= early_b)
                    def _():
                        start_pair(*u_copies(c))
                    return 0
                lax.fori_loop(0, CHUNKS, renorm_u, 0)

                def early_u(side, slot):
                    def body(b, _):
                        z = ez_b[side, pl.ds(pl.multiple_of(b * half_w, half_w), half_w), :]
                        u[slot, b] = norm_relu(z, 0).astype(BF16)
                        return 0
                    return body
                up, down = early_b_copies()
                take_early(up, down, early_u(0, 0), early_u(1, 2), EARLY_B)
                sent_early(up, down)
                clear_moments()

                def mid_body(c, _):
                    @pl.when(c >= early_b)
                    def _():
                        wait_halo(u_copies, c)
                    rows_at = pl.ds(pl.multiple_of(c * m_rows, m_rows), m_rows)
                    sl = pl.ds(c * per_chunk, per_chunk)
                    x = jnp.concatenate([u[r, sl].reshape(m_rows, chan_m) for r in range(3)], axis=1)
                    z = dot(x, wmid[j, :, chan_m:2 * chan_m])
                    z = z + from_left(dot(x, wmid[j, :, 0:chan_m]), half_w)
                    z = z + from_right(dot(x, wmid[j, :, 2 * chan_m:3 * chan_m]), half_w)
                    zb[rows_at, 0:chan_m] = z
                    add_moments(z, 0)
                    return 0
                lax.fori_loop(0, CHUNKS, mid_body, 0)
                send_moments(ar_mid + j, 0)
                wait_sends(u_copies, early_b)
                recv_moments(ar_mid + j, bn_mid[j], 0, count_b)

                clear_moments()
                for t in range(tiles):
                    cols = slice(t * TILE, (t + 1) * TILE)

                    def out_body(c, _):
                        rows_at = pl.ds(c * (points // OUT_STEPS), points // OUT_STEPS)
                        if t == 0:
                            u2[rows_at, :] = norm_relu(zb[rows_at, 0:chan_m], 0).astype(BF16)
                        z = dot(u2[rows_at, :], wout[j, :, cols])
                        zb[rows_at, cols] = z
                        add_moments(z, t * TILE)
                        return 0
                    for c in range(OUT_STEPS):
                        out_body(c, 0)
                    for ts in messages:
                        if t == ts[-1]:
                            send_tiles(ar_out + (j + 1) * tiles, ts)
                    if t == 0:
                        @pl.when(j == blocks - 1)
                        def _():
                            u2_copy().start()
                return 0
            lax.fori_loop(0, blocks, block, 0)

            for t in range(tiles):
                recv_tile(blocks, t)
            nrm_copy = pltpu.make_async_copy(nrm, nrm_out, sem_out.at[2])
            nrm_copy.start()
            h_copy().wait()
            u2_copy().wait()
            nrm_copy.wait()

        scratch = [
            pltpu.VMEM((4, batch, width, chan_a), BF16),
            pltpu.VMEM((3, batch, half_w, chan_m), BF16),
            pltpu.VMEM((points, chan_b), F32),
            pltpu.VMEM((points, chan_b), BF16),
            pltpu.VMEM((points, chan_m), BF16),
            pltpu.VMEM((layers, 4 * chan_a, 6 * chan_a), BF16),
            pltpu.VMEM((9 * chan_a, chan_b), BF16),
            pltpu.VMEM((blocks, chan_b, chan_m), BF16),
            pltpu.VMEM((blocks, 3 * chan_m, 3 * chan_m), BF16),
            pltpu.VMEM((blocks, chan_m, chan_b), BF16),
            pltpu.VMEM((2, 8, chan_b), F32),
            pltpu.VMEM((8, chan_b), F32),
            pltpu.VMEM((blocks + 1, 2, chan_b), F32),
            pltpu.VMEM((2, width, chan_a), F32),
            pltpu.VMEM((ar_total, 1, 2 * TILE), F32),
            pltpu.VMEM((ar_total, groups - 1, 1, 2 * TILE), F32),
            pltpu.VMEM((layers - 1, 2, EARLY_A * width, chan_a), F32),
            pltpu.VMEM((EARLY_A * width, chan_a), F32),
            pltpu.VMEM((2, EARLY_B * half_w, chan_m), F32),
            pltpu.SemaphoreType.DMA((5,)),
            pltpu.SemaphoreType.DMA((2, CHUNKS)),
            pltpu.SemaphoreType.DMA((2, CHUNKS)),
            pltpu.SemaphoreType.DMA((2, CHUNKS)),
            pltpu.SemaphoreType.DMA((2, CHUNKS)),
            pltpu.SemaphoreType.DMA((2, CHUNKS)),
            pltpu.SemaphoreType.DMA((ar_total,)),
            pltpu.SemaphoreType.DMA((ar_total,)),
            pltpu.SemaphoreType.DMA((layers + 1, 2)),
            pltpu.SemaphoreType.DMA((layers + 1, 2)),
            pltpu.SemaphoreType.DMA((3,)),
        ]
        return kernel, scratch, points

    def forward(images, w_a, bn_a, w_down, bn_down, w_in, bn_in, w_mid, bn_mid, w_out, bn_out):
        batch, rows, width, chan_a = images.shape
        chan_b, chan_m = w_in.shape[1:]
        kernel, scratch, points = make_kernel(batch, rows, width, chan_a, chan_b, chan_m, w_a.shape[0], w_in.shape[0])
        hbm = pl.BlockSpec(memory_space=pl.ANY)
        vmem = pl.BlockSpec(memory_space=pltpu.VMEM)
        h_last, branch, moments = pl.pallas_call(
            kernel,
            out_shape=(jax.ShapeDtypeStruct((points, chan_b), BF16),
                       jax.ShapeDtypeStruct((points, chan_m), BF16),
                       jax.ShapeDtypeStruct((8, chan_b), F32)),
            in_specs=[hbm] * 6 + [vmem] * 5,
            out_specs=(hbm, hbm, hbm),
            scratch_shapes=scratch,
            name="conv_stack",
            compiler_params=pltpu.CompilerParams(collective_id=0, has_side_effects=True, vmem_limit_bytes=67043328),
        )(images, w_a, w_down, w_in, w_mid, w_out, bn_a, bn_down, bn_in, bn_mid, bn_out)

        step = points // LAST_STEPS
        last = w_out.shape[0] - 1

        def finish(branch_ref, h_ref, w_ref, nrm_ref, out_ref):
            for t in range(chan_b // TILE):
                cols = slice(t * TILE, (t + 1) * TILE)
                z = jnp.dot(branch_ref[...], w_ref[0, :, cols], preferred_element_type=F32)
                normed = (z - nrm_ref[0:1, cols]) * nrm_ref[1:2, cols] + nrm_ref[2:3, cols]
                out_ref[:, cols] = jnp.maximum(normed + h_ref[:, cols].astype(F32), 0.0).astype(BF16)

        res = pl.pallas_call(
            finish,
            grid=(LAST_STEPS,),
            out_shape=jax.ShapeDtypeStruct((points, chan_b), BF16),
            in_specs=[pl.BlockSpec((step, chan_m), lambda i: (i, 0)),
                      pl.BlockSpec((step, chan_b), lambda i: (i, 0)),
                      pl.BlockSpec((1, chan_m, chan_b), lambda i: (last, 0, 0)),
                      pl.BlockSpec((8, chan_b), lambda i: (0, 0))],
            out_specs=pl.BlockSpec((step, chan_b), lambda i: (i, 0)),
            name="last_norm",
        )(branch, h_last, w_out, moments)
        return res.reshape(batch, rows // 2, width // 2, chan_b)

    act_spec = P("dp", "sp", None, None)
    return jax.shard_map(forward, mesh=mesh, in_specs=(act_spec,) + (P(),) * 10, out_specs=act_spec, check_vma=False)
```
